32 devices in a mesh: pole: 2 (over y), row: 8 (over z, x), col: 2 (over core).
Axes of the slice: x: 2, y: 2, z: 4, core: 2. Of those that a mesh axis runs over, the one named last changes fastest.
Arguments:
- known_inverse: float32 [16, 128, 1024], P('pole', 'col', 'row'), parts along dimension 0, may hold values from -1 to 3, as said below
- first_factor: float32 [2048, 512], P(('pole', 'row')), parts along dimension 0, may hold values from -0.5 to 0.5
- first_corner: float32 [1024, 512], P('pole'), parts along dimension 0, may hold values from -1 to 5, as said below
- first_ancestors: int32 [1024], P('pole'), parts along dimension 0, may hold values from 0 to 1023, as said below
- second_factor: float32 [2048, 512], P(('pole', 'row')), parts along dimension 0, may hold values from -0.75 to 0.75
- second_link: float32 [1024, 512], P('pole'), parts along dimension 0, may hold values from -0.25 to 0.25
- second_corner: float32 [1024, 512], P('pole', 'col'), parts along dimension 0, may hold values from -1 to 5, as said below
- second_ancestors: int32 [512], P('pole'), parts along dimension 0, may hold values from 0 to 1023, as said below
Outputs:
- first_column: float32 [2048, 512], P(('pole', 'row'), 'col'), parts along dimension 0
- first_diagonal: float32 [1024, 512], P('pole', 'col'), parts along dimension 0
- second_column: float32 [2048, 512], P(('pole', 'row'), 'col'), parts along dimension 0
- second_cross: float32 [1024, 512], P('pole', 'col'), parts along dimension 0
- second_diagonal: float32 [1024, 512], P('pole', 'col'), parts along dimension 0
The draws below stay inside these ranges and needn't reach their ends.
There are 2 independent parts, one for each index of `pole`. The reference program is written for one: setup_inputs(seed, part) draws one part's arguments, and reference() takes and returns one part's arrays. A program takes and returns all parts, laid end to end along the dimension named above; each array names one. Nothing has to cross between parts.
Inputs may be any that keep to these rules, and one draw needn't show every extreme that they name: `known_inverse`: K is symmetric. `first_corner`: symmetric. `second_corner`: symmetric. `first_ancestors`: distinct row numbers; every block of 128 consecutive row numbers starting at a multiple of 128 holds at least one of them. `second_ancestors`: distinct row numbers, each of which is also in first_ancestors; every block of 128 consecutive row numbers starting at a multiple of 128 holds at least one of them.
All inputs are finite; a program needn't handle non-finite values.
Results may differ from the reference program's by a relative error of at most 0.000084.
Values sent between devices are 32-bit elements; how exact they have to be, the bound alone decides.
A program may use at most 128 MiB of HBM per device.

```python
import jax
import jax.numpy as jnp
from jax import lax

BLOCK_ROWS = 128
WIDTH = 512
ANC_ROWS = 1024
FIRST_ANC = 512
SECOND_ANC = 256
N_ROW = 8


def symmetric_draw(key, order, lowest, highest, spread):
    noise_key, middle_key = jax.random.split(key)
    noise = jnp.clip(jax.random.normal(noise_key, (order, order), jnp.float32), -4.0, 4.0) * (spread / order ** 0.5)
    middle = jax.random.uniform(middle_key, (order,), jnp.float32, lowest, highest)
    return (noise + noise.T) * 0.5 + jnp.diag(middle)


def draw_known_inverse(key, part):
    whole = symmetric_draw(jax.random.fold_in(key, 3), ANC_ROWS, 0.5, 2.0, 0.5)
    return whole.reshape(N_ROW, BLOCK_ROWS, ANC_ROWS)


def draw_first_corner(key, part):
    return symmetric_draw(jax.random.fold_in(key, 5), WIDTH, 1.0, 3.0, 0.5)


def draw_second_corner(key, part):
    return symmetric_draw(jax.random.fold_in(key, 7), WIDTH, 1.0, 3.0, 0.5)


def ancestor_sets(key):
    numbers = jnp.arange(ANC_ROWS, dtype=jnp.int32)
    places = jax.random.randint(jax.random.fold_in(key, 20), (N_ROW,), 0, BLOCK_ROWS, dtype=jnp.int32)
    keeper = (numbers % BLOCK_ROWS == places[numbers // BLOCK_ROWS]).astype(jnp.int32)
    scores = keeper * ANC_ROWS + jax.random.randint(jax.random.fold_in(key, 21), (ANC_ROWS,), 0, ANC_ROWS, dtype=jnp.int32)
    chosen = jnp.sort(lax.top_k(scores * ANC_ROWS + numbers, FIRST_ANC)[1]).astype(jnp.int32)
    inner = jnp.arange(FIRST_ANC, dtype=jnp.int32)
    inner_scores = keeper[chosen] * ANC_ROWS + jax.random.randint(jax.random.fold_in(key, 22), (FIRST_ANC,), 0, ANC_ROWS, dtype=jnp.int32)
    subset = jnp.sort(chosen[lax.top_k(inner_scores * FIRST_ANC + inner, SECOND_ANC)[1]]).astype(jnp.int32)
    return (chosen, subset)


def draw_first_ancestors(key, part):
    return ancestor_sets(key)[0]


def draw_second_ancestors(key, part):
    return ancestor_sets(key)[1]


def levels(own_key, shape, pieces, least, high):
    gain, own = 1.0, jax.random.fold_in(own_key, 6)
    for axis_at, parts in pieces:
        draws = jnp.exp(jax.random.uniform(jax.random.fold_in(own, axis_at), (parts,), jnp.float32, least / len(pieces), high / len(pieces)))
        gain = gain * jnp.repeat(draws, shape[axis_at] // parts).reshape([-1 if axis == axis_at else 1 for axis in range(len(shape))])
    return gain


def bell_draw(own_key, extent, scale, most, shards=(), kind=jnp.bfloat16):
    array = scale * jax.random.normal(own_key, extent, jnp.float32)
    if shards:
        array = array * levels(own_key, extent, shards, -0.22, 0.18)
    return jnp.clip(array, -most, most).astype(kind)


def setup_inputs(seed: int = 0, part: int = 0) -> dict:
    key_of = jax.random.split(jax.random.key(seed), 9)
    part_keys = jax.random.split(jax.random.fold_in(key_of[8], part), 9)
    known_inverse = draw_known_inverse(jax.random.fold_in(jax.random.fold_in(key_of[8], part), 71), part)
    first_factor = bell_draw(part_keys[1], (ANC_ROWS, WIDTH), (FIRST_ANC // 4) ** -0.5, 0.5, ((0, 8),), jnp.float32)
    first_corner = draw_first_corner(jax.random.fold_in(jax.random.fold_in(key_of[8], part), 71), part)
    first_ancestors = draw_first_ancestors(jax.random.fold_in(jax.random.fold_in(key_of[8], part), 71), part)
    second_factor = bell_draw(part_keys[4], (ANC_ROWS, WIDTH), (SECOND_ANC // 4) ** -0.5, 0.75, ((0, 8),), jnp.float32)
    second_link = bell_draw(part_keys[5], (WIDTH, WIDTH), WIDTH ** -0.5, 0.25, (), jnp.float32)
    second_corner = draw_second_corner(jax.random.fold_in(jax.random.fold_in(key_of[8], part), 71), part)
    second_ancestors = draw_second_ancestors(jax.random.fold_in(jax.random.fold_in(key_of[8], part), 71), part)
    return {"known_inverse": known_inverse, "first_factor": first_factor, "first_corner": first_corner, "first_ancestors": first_ancestors, "second_factor": second_factor, "second_link": second_link, "second_corner": second_corner, "second_ancestors": second_ancestors}


HIGH = lax.Precision.HIGHEST


def product(left, right):
    return jnp.dot(left, right, precision=HIGH, preferred_element_type=jnp.float32)


def transposed_product(left, right):
    return lax.dot_general(left, right, (((0,), (0,)), ((), ())), precision=HIGH, preferred_element_type=jnp.float32)


def row_mask(ancestors):
    return jnp.zeros((ANC_ROWS,), jnp.float32).at[ancestors].set(1.0)[:, None]


def reference(known_inverse, first_factor, first_corner, first_ancestors, second_factor, second_link, second_corner, second_ancestors):
    columns = known_inverse.reshape(ANC_ROWS, ANC_ROWS)
    first_mask = row_mask(first_ancestors)
    second_mask = row_mask(second_ancestors)
    first_masked = first_factor * first_mask
    second_masked = second_factor * second_mask
    first_column = -(transposed_product(columns, first_masked) * first_mask)
    first_diagonal = first_corner - transposed_product(first_masked, first_column)
    second_column = -((transposed_product(columns, second_masked) + product(first_column, second_link)) * second_mask)
    second_cross = -(transposed_product(first_column, second_masked) + product(first_diagonal, second_link))
    second_diagonal = second_corner - transposed_product(second_masked, second_column) - transposed_product(second_link, second_cross)
    return (first_column, first_diagonal, second_column, second_cross, second_diagonal)
```

```python
import functools

import jax
import jax.numpy as jnp
from jax import lax
from jax.experimental import pallas as pl
from jax.experimental.pallas import tpu as pltpu
from jax.sharding import PartitionSpec as P

HIGH = lax.Precision.HIGHEST
MESH = pl.DeviceIdType.MESH
RAILS = 2
CHUNK = 64
LEAD = 3
LAG = 4
VMEM_FOR_WHOLE = 40 * 2**20


def product(left, right):
    return jnp.dot(left, right, precision=HIGH, preferred_element_type=jnp.float32)


def transposed_product(left, right):
    return lax.dot_general(
        left, right, (((0,), (0,)), ((), ())), precision=HIGH, preferred_element_type=jnp.float32
    )


def local_mask(ancestors, row_start, block_rows):
    global_rows = row_start + jnp.arange(block_rows, dtype=jnp.int32)
    return jnp.any(ancestors[:, None] == global_rows[None, :], axis=0).astype(jnp.float32)[:, None]


def on_device_collectives(
    known_inverse,
    first_factor,
    first_corner,
    first_ancestors,
    second_factor,
    second_link,
    second_corner,
    second_ancestors,
):
    groups, share_rows, block_rows = known_inverse.shape
    half_width = second_corner.shape[1]
    col_index = lax.axis_index("col")
    row_start = lax.axis_index("row") * block_rows
    first_mask = local_mask(first_ancestors, row_start, block_rows)
    second_mask = local_mask(second_ancestors, row_start, block_rows)
    first_masked = first_factor * first_mask
    second_masked = second_factor * second_mask
    share_start = col_index * share_rows
    first_piece = lax.dynamic_slice_in_dim(first_masked, share_start, share_rows, 0)
    second_piece = lax.dynamic_slice_in_dim(second_masked, share_start, share_rows, 0)
    columns = known_inverse.reshape(groups * share_rows, block_rows)

    def add_piece(piece):
        return transposed_product(columns, piece)

    first_partial = add_piece(lax.all_gather(first_piece, "row", axis=0, tiled=True))
    second_partial = add_piece(lax.all_gather(second_piece, "row", axis=0, tiled=True))
    first_image = lax.psum_scatter(first_partial, "col", scatter_dimension=1, tiled=True)
    first_column = -(first_image * first_mask)
    first_full = lax.all_gather(first_column, "col", axis=1, tiled=True)
    diagonal_partial = transposed_product(first_masked, first_column)
    corner_half = lax.dynamic_slice_in_dim(first_corner, col_index * half_width, half_width, 1)
    first_diagonal = corner_half - lax.psum(diagonal_partial, "row")
    diagonal_full = lax.all_gather(first_diagonal, "col", axis=1, tiled=True)
    second_image = lax.psum_scatter(second_partial, "col", scatter_dimension=1, tiled=True)
    link_half = lax.dynamic_slice_in_dim(second_link, col_index * half_width, half_width, 1)
    second_column = -((second_image + product(first_full, link_half)) * second_mask)
    second_half = lax.dynamic_slice_in_dim(second_masked, col_index * half_width, half_width, 1)
    cross_partial = transposed_product(first_full, second_half)
    closing_partial = transposed_product(second_masked, second_column)
    cross_total, closing_total = lax.psum((cross_partial, closing_partial), "row")
    second_cross = -(cross_total + product(diagonal_full, link_half))
    second_diagonal = second_corner - closing_total - transposed_product(second_link, second_cross)
    return (first_column, first_diagonal, second_column, second_cross, second_diagonal)


def split(value):
    high = value.astype(jnp.bfloat16)
    return high, (value - high.astype(jnp.float32)).astype(jnp.bfloat16)


def dot(left, right):
    return jnp.dot(left, right, preferred_element_type=jnp.float32)


def dot3(left, right):
    (left_high, left_low), (right_high, right_low) = left, right
    return dot(left_high, right_high) + (dot(left_low, right_high) + dot(left_high, right_low))


def chain_kernel(
    n,
    known,
    factor_one,
    corner_one,
    ancestors_one,
    factor_two,
    link,
    corner_two,
    ancestors_two,
    column_one,
    diagonal_one,
    column_two,
    cross_two,
    diagonal_two,
    k_raw,
    stage,
    raw,
    k_part,
    k_peer,
    k_full,
    select,
    own,
    inward,
    outward,
    total,
    link_buf,
    corner_buf,
    corner_two_buf,
    link_split,
    reduced,
    both,
    both_t,
    mine_split,
    k_split,
    local_sem,
    raw_send,
    raw_recv,
    hop_send,
    hop_recv,
    side_send,
    side_recv,
    pair_send,
    pair_recv,
):
    f32, bf16 = jnp.float32, jnp.bfloat16
    levels = n // RAILS
    groups, share, block = k_raw.shape
    width = link_buf.shape[0]
    hw, quarter = width // 2, width // 4
    one, two = ancestors_one.shape[1], ancestors_two.shape[1]
    rows_all = own.shape[0]
    chunks = rows_all // CHUNK
    part = one // 4
    k_start = one + two

    me_row, me_col = lax.axis_index("row"), lax.axis_index("col")
    level, rail = me_row // RAILS, lax.rem(me_row, RAILS)
    other_rail, other_col = 1 - rail, 1 - me_col
    my_quarter = 2 * me_col + rail
    side_quarter = 2 * me_col + other_rail
    near = jnp.where(level < levels // 2, 0, 1)
    far = 1 - near
    step = 1 - 2 * near
    inner = jnp.logical_and(level > 0, level < levels - 1)
    outer = jnp.logical_not(inner)
    near_row = (level + step) * RAILS + rail
    far_row = (level - step) * RAILS + rail
    side_row = level * RAILS + other_rail

    barrier = pltpu.get_barrier_semaphore()

    def greet(**place):
        pl.semaphore_signal(barrier, inc=1, device_id=place, device_id_type=MESH)

    greet(col=other_col)
    greet(row=side_row)
    greet(row=near_row)

    @pl.when(inner)
    def _():
        greet(row=far_row)

    count = [0]

    def local(src, dst):
        copy = pltpu.make_async_copy(src, dst, local_sem.at[count[0]])
        count[0] += 1
        copy.start()
        return copy

    def lanes(which):
        return pl.ds(pl.multiple_of(which * quarter, 128), quarter)

    f_stage = [
        local(factor.at[:, lanes(side_quarter)], stage.at[i])
        for i, factor in enumerate((factor_one, factor_two))
    ]
    f_own = [
        local(factor.at[:, lanes(my_quarter)], raw.at[i, rail])
        for i, factor in enumerate((factor_one, factor_two))
    ]
    k_own = local(known, k_raw)
    rest = [local(link, link_buf), local(corner_one, corner_buf), local(corner_two, corner_two_buf)]

    def remote(src, dst, send, recv, **place):
        return pltpu.make_async_remote_copy(
            src_ref=src, dst_ref=dst, send_sem=send, recv_sem=recv, device_id=place, device_id_type=MESH
        )

    def raw_copy(i):
        src = stage.at[i] if i < 2 else k_full.at[:, lanes(side_quarter)]
        return remote(src, raw.at[i, rail], raw_send.at[i], raw_recv.at[i], row=side_row)

    def k_copy():
        return remote(k_part, k_peer, raw_send.at[3], raw_recv.at[3], col=other_col)

    def rows_of(k):
        return pl.ds(pl.multiple_of(k * CHUNK, CHUNK), CHUNK)

    def hop(direction, k, src, row):
        return remote(
            src.at[rows_of(k)],
            inward.at[direction, rows_of(k)],
            hop_send.at[direction, k],
            hop_recv.at[direction, k],
            row=row,
        )

    def side_copy(k):
        at = total.at[my_quarter, rows_of(k)]
        return remote(at, at, side_send.at[k], side_recv.at[k], row=side_row)

    def pair_copy(which, k):
        at = total.at[my_quarter if which == 0 else side_quarter, rows_of(k)]
        return remote(at, at, pair_send.at[which, k], pair_recv.at[which, k], col=other_col)

    def numbers(ancestors):
        wide = jnp.broadcast_to(ancestors[...].astype(f32), (128, ancestors.shape[1]))
        return wide.T

    def selection(column):
        lane = lax.broadcasted_iota(jnp.int32, (column.shape[0], RAILS * block), 1) + level * (RAILS * block)
        repeated = jnp.concatenate([column] * (RAILS * block // 128), axis=1)
        return jnp.where(repeated == lane.astype(f32), 1.0, 0.0).astype(bf16)

    column = numbers(ancestors_one)
    select[:one, :] = selection(column)
    select[one:, :] = selection(numbers(ancestors_two))

    for copy in f_stage:
        copy.wait()
    pl.semaphore_wait(barrier, 3 + inner.astype(jnp.int32))
    raw_copy(0).start()
    raw_copy(1).start()

    k_own.wait()
    at = (
        lax.broadcasted_iota(jnp.int32, (groups, share, one), 0) * block
        + lax.broadcasted_iota(jnp.int32, (groups, share, one), 1)
        + me_col * share
    )
    pick = jnp.where(at == ancestors_one[...].reshape(1, 1, one), 1.0, 0.0).astype(bf16)
    k_high, k_low = split(k_raw[...].reshape(groups * share, block).T)
    stacked = dot(jnp.concatenate([k_high, k_low], axis=0), pick.reshape(groups * share, one))
    k_part[...] = stacked[:block] + stacked[block:]
    k_copy().start()

    def place(i, chosen):
        high, low = split(raw[i].reshape(RAILS * block, quarter))
        wide = dot(chosen, jnp.concatenate([high, low], axis=1))
        return wide[:, :quarter] + wide[:, quarter:]

    def send_own(first, last):
        @pl.when(outer)
        def _():
            for k in range(first // CHUNK, last // CHUNK):
                hop(near, k, own, near_row).start()

    for copy in f_own:
        copy.wait()
    raw_copy(0).wait_recv()
    own[:one, :] = place(0, select[:one, :])
    send_own(0, one)
    k_copy().wait_recv()
    k_full[...] = k_part[...] + k_peer[...]
    raw[2, rail] = k_full[:, lanes(my_quarter)]
    raw_copy(2).start()
    raw_copy(1).wait_recv()
    own[one:k_start, :] = place(1, select[one:, :])
    send_own(one, k_start)

    def near_event(k):
        @pl.when(inner)
        def _():
            hop(near, k, own, near_row).wait_recv()
            outward[near, rows_of(k)] = own[rows_of(k)] + inward[near, rows_of(k)]
            hop(near, k, outward.at[near], near_row).start()

    def far_event(k):
        hop(far, k, own, far_row).wait_recv()
        passed = own[rows_of(k)] + inward[far, rows_of(k)]

        @pl.when(inner)
        def _():
            outward[far, rows_of(k)] = passed
            hop(far, k, outward.at[far], far_row).start()
            total[my_quarter, rows_of(k)] = passed + inward[near, rows_of(k)]

        @pl.when(outer)
        def _():
            total[my_quarter, rows_of(k)] = passed

        side_copy(k).start()
        pair_copy(0, k).start()

    def relay(k):
        side_copy(k).wait_recv()
        pair_copy(1, k).start()

    def events(first, last):
        def body(k, carry):
            far_event(k)

            @pl.when(k + LEAD < chunks)
            def _():
                near_event(k + LEAD)

            @pl.when(k >= LAG)
            def _():
                relay(k - LAG)

            return carry

        lax.fori_loop(first, last, body, 0)

    def relays(first, last):
        def body(k, carry):
            relay(k)
            return carry

        lax.fori_loop(first, last, body, 0)

    def paired(first, last):
        def body(k, carry):
            pair_copy(0, k).wait_recv()
            pair_copy(1, k).wait_recv()
            return carry

        lax.fori_loop(first // CHUNK, last // CHUNK, body, 0)

    def mine(ref, start):
        return ref[:, pl.ds(pl.multiple_of(start + me_col * hw, 128), hw)]

    for k in range(LEAD):
        near_event(k)
    raw_copy(2).wait_recv()
    high, low = split(raw[2].reshape(RAILS * block, quarter))
    halves = jnp.concatenate([high, low], axis=1)
    for i in range(3):
        chosen = select[pl.ds(pl.multiple_of(lax.rem(my_quarter + i, 4) * part, part), part), :]
        wide = dot(chosen, halves)
        own[k_start + i * part : k_start + (i + 1) * part, :] = wide[:, :quarter] + wide[:, quarter:]
    send_own(k_start, rows_all)

    for copy in rest:
        copy.wait()
    link_split[0], link_split[1] = split(link_buf[...])
    half_split = split(mine(link_buf, 0))
    corner_link = dot3(split(corner_buf[...]), half_split)
    cross_two[...] = -corner_link
    diagonal_one[...] = mine(corner_buf, 0)
    diagonal_two[...] = corner_two_buf[...] + dot3(split(link_buf[...].T), split(corner_link))

    ready = min(chunks, one // CHUNK + LAG + 1)
    events(0, ready)
    paired(0, one)
    first = jnp.concatenate([total[q, :one, :] for q in range(4)], axis=1)
    first_split = split(first)
    both[0, :, :width], both[1, :, :width] = first_split
    both_t[0, :width, :], both_t[1, :width, :] = split(first.T)
    events(ready, chunks)
    reduced[...] = dot3(first_split, (link_split[0], link_split[1]))
    relays(chunks - LAG, chunks)

    paired(one, k_start)
    same = jnp.concatenate([column] * (two // 128), axis=1) == ancestors_two[...].astype(f32)
    spread = jnp.where(same, 1.0, 0.0).astype(bf16)
    second_high, second_low = split(jnp.concatenate([total[q, one:k_start, :] for q in range(4)], axis=1))
    second = dot(spread, second_high) + dot(spread, second_low) - reduced[...]
    both[0, :, width:], both[1, :, width:] = split(second)
    both_t[0, width:, :], both_t[1, width:, :] = split(second.T)
    for i in range(2):
        mine_split[i] = jnp.concatenate([mine(both.at[i], 0), mine(both.at[i], width)], axis=1)

    def mask_of(ancestors):
        rows = me_row * block + lax.broadcasted_iota(jnp.int32, (block, ancestors.shape[1]), 0)
        return jnp.max(jnp.where(rows == ancestors[...], 1.0, 0.0), axis=1, keepdims=True)

    mine_both = (mine_split[0], mine_split[1])
    image = dot3(split(k_full[...]), mine_both)
    column_one[...] = -(image[:, :hw] * mask_of(ancestors_one))
    column_two[...] = -(image[:, hw:] * mask_of(ancestors_two))

    def put(row, col, value):
        at = (slice(row * part, (row + 1) * part), slice(col * part, (col + 1) * part))
        k_split[(0, *at)], k_split[(1, *at)] = split(value)

    paired(k_start, rows_all)
    for q in range(4):
        for i in range(3):
            value = total[q, k_start + i * part : k_start + (i + 1) * part, :]
            put((q + i) % 4, q, value)
            if i == 1:
                put(q, (q + 1) % 4, value.T)
    grown = split(dot3((k_split[0], k_split[1]), mine_both))
    upper = dot3((both_t[0, :width, :], both_t[1, :width, :]), grown)
    diagonal_one[...] += upper[:, :hw]
    cross_two[...] += upper[:, hw:]
    diagonal_two[...] += dot3(
        (both_t[0, width:, :], both_t[1, width:, :]), (grown[0][:, hw:], grown[1][:, hw:])
    )

    for i in range(3):
        raw_copy(i).wait_send()
    k_copy().wait_send()

    def sent(k, carry):
        hop(near, k, own, near_row).wait_send()

        @pl.when(inner)
        def _():
            hop(far, k, own, far_row).wait_send()

        side_copy(k).wait_send()
        pair_copy(0, k).wait_send()
        pair_copy(1, k).wait_send()
        return carry

    lax.fori_loop(0, chunks, sent, 0)


def place_kernel(*refs):
    for source, target in zip(refs[:5], refs[5:]):
        target[...] = source[...]


def on_device_chain(
    n,
    known_inverse,
    first_factor,
    first_corner,
    first_ancestors,
    second_factor,
    second_link,
    second_corner,
    second_ancestors,
):
    groups, share, block = known_inverse.shape
    width = second_link.shape[0]
    hw, quarter = second_corner.shape[1], width // 4
    one, two = first_ancestors.shape[0], second_ancestors.shape[0]
    rows_all = one + two + 3 * (one // 4)
    chunks = rows_all // CHUNK
    f32, bf16 = jnp.float32, jnp.bfloat16
    anywhere = pl.BlockSpec(memory_space=pl.ANY)
    vmem = pl.BlockSpec(memory_space=pltpu.VMEM)
    square = jax.ShapeDtypeStruct((width, hw), f32)
    column = jax.ShapeDtypeStruct((block, hw), f32)
    results = pl.pallas_call(
        functools.partial(chain_kernel, n),
        out_shape=(column, square, column, square, square),
        in_specs=[anywhere, anywhere, anywhere, vmem, anywhere, anywhere, anywhere, vmem],
        out_specs=(vmem,) * 5,
        scratch_shapes=[
            pltpu.VMEM((groups, share, block), f32),
            pltpu.VMEM((2, block, quarter), f32),
            pltpu.VMEM((3, RAILS, block, quarter), f32),
            pltpu.VMEM((block, one), f32),
            pltpu.VMEM((block, one), f32),
            pltpu.VMEM((block, one), f32),
            pltpu.VMEM((one + two, RAILS * block), bf16),
            pltpu.VMEM((rows_all, quarter), f32),
            pltpu.VMEM((2, rows_all, quarter), f32),
            pltpu.VMEM((2, rows_all, quarter), f32),
            pltpu.VMEM((4, rows_all, quarter), f32),
            pltpu.VMEM((width, width), f32),
            pltpu.VMEM((width, width), f32),
            pltpu.VMEM((width, hw), f32),
            pltpu.VMEM((2, width, width), bf16),
            pltpu.VMEM((one, width), f32),
            pltpu.VMEM((2, one, 2 * width), bf16),
            pltpu.VMEM((2, 2 * width, one), bf16),
            pltpu.VMEM((2, one, 2 * hw), bf16),
            pltpu.VMEM((2, one, one), bf16),
            pltpu.SemaphoreType.DMA((8,)),
            pltpu.SemaphoreType.DMA((4,)),
            pltpu.SemaphoreType.DMA((4,)),
            pltpu.SemaphoreType.DMA((2, chunks)),
            pltpu.SemaphoreType.DMA((2, chunks)),
            pltpu.SemaphoreType.DMA((chunks,)),
            pltpu.SemaphoreType.DMA((chunks,)),
            pltpu.SemaphoreType.DMA((2, chunks)),
            pltpu.SemaphoreType.DMA((2, chunks)),
        ],
        compiler_params=pltpu.CompilerParams(collective_id=0, has_side_effects=True),
    )(
        known_inverse,
        first_factor,
        first_corner,
        first_ancestors.reshape(1, -1),
        second_factor,
        second_link,
        second_corner,
        second_ancestors.reshape(1, -1),
    )
    return pl.pallas_call(
        place_kernel,
        out_shape=(column, square, column, square, square),
        in_specs=[vmem] * 5,
        out_specs=(vmem,) * 5,
    )(*results)


def solution(mesh):
    def on_device(*args):
        n = mesh.shape["row"]
        groups, share, block = args[0].shape
        width = args[5].shape[0]
        one, two = args[3].shape[0], args[7].shape[0]
        held = 4 * (one + two + 3 * (one // 4)) * (width // 4) * 9 + 16 * one * (width + one)
        fits = (
            mesh.shape["col"] == 2
            and n % (2 * RAILS) == 0
            and groups == n
            and block == 2 * share
            and block % 128 == 0
            and one == width
            and width % 512 == 0
            and two % 128 == 0
            and held <= VMEM_FOR_WHOLE
        )
        return on_device_chain(n, *args) if fits else on_device_collectives(*args)

    return jax.shard_map(
        on_device,
        mesh=mesh,
        in_specs=(
            P("pole", "col", "row"),
            P(("pole", "row"), None),
            P("pole", None),
            P("pole"),
            P(("pole", "row"), None),
            P("pole", None),
            P("pole", "col"),
            P("pole"),
        ),
        out_specs=(
            P(("pole", "row"), "col"),
            P("pole", "col"),
            P(("pole", "row"), "col"),
            P("pole", "col"),
            P("pole", "col"),
        ),
        check_vma=False,
    )
```

```python
import functools

import jax
import jax.numpy as jnp
from jax import lax
from jax.experimental import pallas as pl
from jax.experimental.pallas import tpu as pltpu
from jax.sharding import PartitionSpec as P

HIGH = lax.Precision.HIGHEST
MESH = pl.DeviceIdType.MESH
RAILS = 2
LEVELS = 4
CHUNK = 128
LAG = 3
VMEM_FOR_WHOLE = 40 * 2**20


def product(left, right):
    return jnp.dot(left, right, precision=HIGH, preferred_element_type=jnp.float32)


def transposed_product(left, right):
    return lax.dot_general(
        left, right, (((0,), (0,)), ((), ())), precision=HIGH, preferred_element_type=jnp.float32
    )


def local_mask(ancestors, row_start, block_rows):
    global_rows = row_start + jnp.arange(block_rows, dtype=jnp.int32)
    return jnp.any(ancestors[:, None] == global_rows[None, :], axis=0).astype(jnp.float32)[:, None]


def on_device_collectives(
    known_inverse,
    first_factor,
    first_corner,
    first_ancestors,
    second_factor,
    second_link,
    second_corner,
    second_ancestors,
):
    groups, share_rows, block_rows = known_inverse.shape
    half_width = second_corner.shape[1]
    col_index = lax.axis_index("col")
    row_start = lax.axis_index("row") * block_rows
    first_mask = local_mask(first_ancestors, row_start, block_rows)
    second_mask = local_mask(second_ancestors, row_start, block_rows)
    first_masked = first_factor * first_mask
    second_masked = second_factor * second_mask
    share_start = col_index * share_rows
    first_piece = lax.dynamic_slice_in_dim(first_masked, share_start, share_rows, 0)
    second_piece = lax.dynamic_slice_in_dim(second_masked, share_start, share_rows, 0)
    columns = known_inverse.reshape(groups * share_rows, block_rows)

    def add_piece(piece):
        return transposed_product(columns, piece)

    first_partial = add_piece(lax.all_gather(first_piece, "row", axis=0, tiled=True))
    second_partial = add_piece(lax.all_gather(second_piece, "row", axis=0, tiled=True))
    first_image = lax.psum_scatter(first_partial, "col", scatter_dimension=1, tiled=True)
    first_column = -(first_image * first_mask)
    first_full = lax.all_gather(first_column, "col", axis=1, tiled=True)
    diagonal_partial = transposed_product(first_masked, first_column)
    corner_half = lax.dynamic_slice_in_dim(first_corner, col_index * half_width, half_width, 1)
    first_diagonal = corner_half - lax.psum(diagonal_partial, "row")
    diagonal_full = lax.all_gather(first_diagonal, "col", axis=1, tiled=True)
    second_image = lax.psum_scatter(second_partial, "col", scatter_dimension=1, tiled=True)
    link_half = lax.dynamic_slice_in_dim(second_link, col_index * half_width, half_width, 1)
    second_column = -((second_image + product(first_full, link_half)) * second_mask)
    second_half = lax.dynamic_slice_in_dim(second_masked, col_index * half_width, half_width, 1)
    cross_partial = transposed_product(first_full, second_half)
    closing_partial = transposed_product(second_masked, second_column)
    cross_total, closing_total = lax.psum((cross_partial, closing_partial), "row")
    second_cross = -(cross_total + product(diagonal_full, link_half))
    second_diagonal = second_corner - closing_total - transposed_product(second_link, second_cross)
    return (first_column, first_diagonal, second_column, second_cross, second_diagonal)


def split(value):
    high = value.astype(jnp.bfloat16)
    return high, (value - high.astype(jnp.float32)).astype(jnp.bfloat16)


def dot(left, right):
    return jnp.dot(left, right, preferred_element_type=jnp.float32)


def dot3(left, right):
    (left_high, left_low), (right_high, right_low) = left, right
    return dot(left_high, right_high) + (dot(left_low, right_high) + dot(left_high, right_low))


def quad_kernel(
    n,
    known,
    factor_one,
    corner_one,
    ancestors_one,
    factor_two,
    link,
    corner_two,
    ancestors_two,
    column_one,
    diagonal_one,
    column_two,
    cross_two,
    diagonal_two,
    k_raw,
    stage,
    raw,
    k_part,
    k_peer,
    k_full,
    select,
    pair,
    quad,
    inward,
    outward,
    total,
    link_buf,
    corner_buf,
    corner_two_buf,
    link_split,
    reduced,
    both,
    both_t,
    mine_split,
    k_split,
    k_last,
    local_sem,
    k_sem,
    raw_send,
    raw_recv,
    hop_send,
    hop_recv,
    side_send,
    side_recv,
    pair_send,
    pair_recv,
):
    f32, bf16 = jnp.float32, jnp.bfloat16
    groups, share, block = k_raw.shape
    width = link_buf.shape[0]
    hw, quarter = width // 2, width // 4
    one, two = ancestors_one.shape[1], ancestors_two.shape[1]
    rows_all = pair.shape[0]
    chunks = rows_all // CHUNK
    part = one // 4
    k_start = one + two
    common = (k_start + 2 * part) // CHUNK
    pair_rows = RAILS * block

    me_row, me_col = lax.axis_index("row"), lax.axis_index("col")
    level, rail = me_row // RAILS, lax.rem(me_row, RAILS)
    parity = lax.rem(level, 2)
    mate_level = level + 1 - 2 * parity
    other_rail, other_col = 1 - rail, 1 - me_col
    my_quarter = 2 * me_col + rail
    side_quarter = 2 * me_col + other_rail
    my_place = RAILS * parity + rail
    inner = jnp.logical_and(level > 0, level < LEVELS - 1)
    outer = jnp.logical_not(inner)
    extra = me_col == 1
    side_row = level * RAILS + other_rail
    mate_row = mate_level * RAILS + rail
    slant_row = mate_level * RAILS + other_rail
    across_row = (LEVELS - 1 - level) * RAILS + rail

    barrier = pltpu.get_barrier_semaphore()

    def greet(**place):
        pl.semaphore_signal(barrier, inc=1, device_id=place, device_id_type=MESH)

    greet(row=slant_row)
    greet(row=mate_row)
    greet(row=side_row)
    greet(col=other_col)

    @pl.when(inner)
    def _():
        greet(row=across_row)

    count = [0]

    def local(src, dst):
        copy = pltpu.make_async_copy(src, dst, local_sem.at[count[0]])
        count[0] += 1
        copy.start()
        return copy

    def lanes(which):
        return pl.ds(pl.multiple_of(which * quarter, 128), quarter)

    f_copies = [
        [
            local(factor.at[:, lanes(side_quarter)], stage.at[i]),
            local(factor.at[:, lanes(my_quarter)], raw.at[i, my_place]),
        ]
        for i, factor in enumerate((factor_one, factor_two))
    ]
    k_own = local(known, k_raw)
    rest = [local(link, link_buf), local(corner_one, corner_buf), local(corner_two, corner_two_buf)]

    def remote(src, dst, send, recv, **place):
        return pltpu.make_async_remote_copy(
            src_ref=src, dst_ref=dst, send_sem=send, recv_sem=recv, device_id=place, device_id_type=MESH
        )

    def raw_copy(kind, i):
        if kind == 0:
            src = raw.at[i, my_place]
        else:
            src = stage.at[i] if i < 2 else k_full.at[:, lanes(side_quarter)]
        row = (mate_row, side_row, slant_row)[kind]
        return remote(src, raw.at[i, my_place], raw_send.at[kind, i], raw_recv.at[kind, i], row=row)

    def send_raw(i):
        @pl.when(outer)
        def _():
            raw_copy(0, i).start()
            raw_copy(2, i).start()

        raw_copy(1, i).start()

    def wait_raw(i):
        raw_copy(1, i).wait_recv()

        @pl.when(inner)
        def _():
            raw_copy(0, i).wait_recv()
            raw_copy(2, i).wait_recv()

    def k_copy():
        return remote(k_part, k_peer, k_sem.at[0], k_sem.at[1], col=other_col)

    def rows_of(k):
        return pl.ds(pl.multiple_of(k * CHUNK, CHUNK), CHUNK)

    def cross_copy(k):
        at = rows_of(k)
        return remote(quad.at[at], inward.at[at], hop_send.at[0, k], hop_recv.at[k], row=across_row)

    def outer_copy(k):
        at = rows_of(k)
        return remote(outward.at[at], inward.at[at], hop_send.at[1, k], hop_recv.at[k], row=mate_row)

    def side_copy(k):
        at = total.at[my_quarter, rows_of(k)]
        return remote(at, at, side_send.at[k], side_recv.at[k], row=side_row)

    def pair_copy(which, k):
        at = total.at[my_quarter if which == 0 else side_quarter, rows_of(k)]
        return remote(at, at, pair_send.at[which, k], pair_recv.at[which, k], col=other_col)

    def held(k, act, by=extra):
        if isinstance(k, int) and k >= common:

            @pl.when(by)
            def _():
                act(k)
        else:
            act(k)

    def numbers(ancestors):
        wide = jnp.broadcast_to(ancestors[...].astype(f32), (128, ancestors.shape[1]))
        return wide.T

    def selection(column):
        shape = (column.shape[0], 2 * pair_rows)
        lane = lax.broadcasted_iota(jnp.int32, shape, 1) + (level // 2) * (2 * pair_rows)
        repeated = jnp.concatenate([column] * (2 * pair_rows // 128), axis=1)
        return jnp.where(repeated == lane.astype(f32), 1.0, 0.0).astype(bf16)

    column = numbers(ancestors_one)
    select[:one, :] = selection(column)
    select[one:, :] = selection(numbers(ancestors_two))
    k_last[...] = jnp.zeros_like(k_last)

    for copies in f_copies:
        for copy in copies:
            copy.wait()
    pl.semaphore_wait(barrier, 4 + inner.astype(jnp.int32))
    send_raw(0)

    k_own.wait()
    at = (
        lax.broadcasted_iota(jnp.int32, (groups, share, one), 0) * block
        + lax.broadcasted_iota(jnp.int32, (groups, share, one), 1)
        + me_col * share
    )
    pick = jnp.where(at == ancestors_one[...].reshape(1, 1, one), 1.0, 0.0).astype(bf16)
    k_high, k_low = split(k_raw[...].reshape(groups * share, block).T)
    stacked = dot(jnp.concatenate([k_high, k_low], axis=0), pick.reshape(groups * share, one))
    k_part[...] = stacked[:block] + stacked[block:]
    k_copy().start()

    def mine(ref, start):
        return ref[:, pl.ds(pl.multiple_of(start + me_col * hw, 128), hw)]

    for copy in rest:
        copy.wait()
    link_split[0], link_split[1] = split(link_buf[...])
    half_split = split(mine(link_buf, 0))
    corner_link = dot3(split(corner_buf[...]), half_split)
    cross_two[...] = -corner_link
    diagonal_one[...] = mine(corner_buf, 0)
    diagonal_two[...] = corner_two_buf[...] + dot3(split(link_buf[...].T), split(corner_link))

    def contribute(i, pieces):
        def halves(which):
            high, low = split(raw[i, pl.ds(which * RAILS, RAILS)].reshape(pair_rows, quarter))
            return jnp.concatenate([high, low], axis=1)

        def placed(which, value, start, size):
            columns = pl.ds(pl.multiple_of(which * pair_rows, 128), pair_rows)
            wide = dot(select[pl.ds(start, size), columns], value)
            return wide[:, :quarter] + wide[:, quarter:]

        value = halves(parity)
        for to, start, size in pieces:
            pair[to : to + size, :] = placed(parity, value, start, size)

        @pl.when(inner)
        def _():
            value = halves(1 - parity)
            for to, start, size in pieces:
                quad[to : to + size, :] = pair[to : to + size, :] + placed(1 - parity, value, start, size)
            for k in range(pieces[0][0] // CHUNK, (pieces[-1][0] + pieces[-1][2]) // CHUNK):
                held(k, lambda k: cross_copy(k).start())

    wait_raw(0)
    send_raw(1)
    contribute(0, [(0, 0, one)])
    k_copy().wait_recv()
    k_full[...] = k_part[...] + k_peer[...]
    raw[2, my_place] = k_full[:, lanes(my_quarter)]
    send_raw(2)
    wait_raw(1)
    contribute(1, [(one, one, two)])
    wait_raw(2)
    contribute(
        2,
        [
            (k_start + i * part, pl.multiple_of(lax.rem(my_quarter + i, 4) * part, part), part)
            for i in range(3)
        ],
    )

    def far_event(k):
        cross_copy(k).wait_recv()
        at = rows_of(k)

        @pl.when(inner)
        def _():
            outward[at] = pair[at] + inward[at]
            total[my_quarter, at] = quad[at] + inward[at]
            outer_copy(k).start()

        @pl.when(outer)
        def _():
            total[my_quarter, at] = pair[at] + inward[at]

        side_copy(k).start()
        pair_copy(0, k).start()

    def relay(k):
        side_copy(k).wait_recv()
        pair_copy(1, k).start()

    def paired(first, last):
        for k in range(first // CHUNK, last // CHUNK):
            held(k, lambda k: (pair_copy(0, k).wait_recv(), pair_copy(1, k).wait_recv()), me_col == 0)

    def event(k):
        held(k, far_event)
        if k >= LAG:
            held(k - LAG, relay)

    ready = min(chunks, one // CHUNK + LAG + 1)
    for k in range(ready):
        event(k)
    paired(0, one)
    first = jnp.concatenate([total[q, :one, :] for q in range(4)], axis=1)
    first_split = split(first)
    both[0, :, :width], both[1, :, :width] = first_split
    both_t[0, :width, :], both_t[1, :width, :] = split(first.T)
    for k in range(ready, chunks):
        event(k)
    reduced[...] = dot3(first_split, (link_split[0], link_split[1]))

    late = list(range(chunks - LAG, chunks))
    third = -(-LAG // 3)
    for k in late[:third]:
        held(k, relay)
    paired(one, k_start)
    same = jnp.concatenate([column] * (two // 128), axis=1) == ancestors_two[...].astype(f32)
    spread = jnp.where(same, 1.0, 0.0).astype(bf16)
    second_high, second_low = split(jnp.concatenate([total[q, one:k_start, :] for q in range(4)], axis=1))
    second = dot(spread, second_high) + dot(spread, second_low) - reduced[...]
    both[0, :, width:], both[1, :, width:] = split(second)
    both_t[0, width:, :], both_t[1, width:, :] = split(second.T)
    for i in range(2):
        mine_split[i] = jnp.concatenate([mine(both.at[i], 0), mine(both.at[i], width)], axis=1)
    for k in late[third : 2 * third]:
        held(k, relay)

    def mask_of(ancestors):
        rows = me_row * block + lax.broadcasted_iota(jnp.int32, (block, ancestors.shape[1]), 0)
        return jnp.max(jnp.where(rows == ancestors[...], 1.0, 0.0), axis=1, keepdims=True)

    mine_both = (mine_split[0], mine_split[1])
    image = dot3(split(k_full[...]), mine_both)
    column_one[...] = -(image[:, :hw] * mask_of(ancestors_one))
    column_two[...] = -(image[:, hw:] * mask_of(ancestors_two))
    for k in late[2 * third :]:
        held(k, relay)

    def put(row, col, value):
        at = (slice(row * part, (row + 1) * part), slice(col * part, (col + 1) * part))
        k_split[(0, *at)], k_split[(1, *at)] = split(value)

    def put_last(row, value):
        at = (row // 2, slice(row % 2 * part, (row % 2 + 1) * part), slice(row % 2 * part, (row % 2 + 1) * part))
        k_last[(0, *at)], k_last[(1, *at)] = split(value)

    paired(k_start, k_start + 2 * part)
    for q in range(4):
        put(q, q, total[q, k_start : k_start + part, :])
        value = total[q, k_start + part : k_start + 2 * part, :]
        put((q + 1) % 4, q, value)
        put(q, (q + 1) % 4, value.T)
        put(q, (q + 2) % 4, jnp.zeros((part, part), f32))
    reduced[...] = dot3((k_split[0], k_split[1]), mine_both)
    paired(k_start + 2 * part, rows_all)
    for q in range(2):
        value = total[q + 2, k_start + 2 * part :, :]
        put_last(q, value)
        put_last(q + 2, value.T)
    half = one // 2
    last = [
        dot3(
            (k_last[0, i], k_last[1, i]),
            (mine_split[0, (1 - i) * half : (2 - i) * half, :], mine_split[1, (1 - i) * half : (2 - i) * half, :]),
        )
        for i in range(2)
    ]
    grown = split(reduced[...] + jnp.concatenate(last, axis=0))
    upper = dot3((both_t[0, :width, :], both_t[1, :width, :]), grown)
    diagonal_one[...] += upper[:, :hw]
    cross_two[...] += upper[:, hw:]
    diagonal_two[...] += dot3(
        (both_t[0, width:, :], both_t[1, width:, :]), (grown[0][:, hw:], grown[1][:, hw:])
    )

    for i in range(3):
        raw_copy(1, i).wait_send()
    k_copy().wait_send()

    @pl.when(outer)
    def _():
        for i in range(3):
            raw_copy(0, i).wait_send()
            raw_copy(2, i).wait_send()

    def sent(k):
        @pl.when(inner)
        def _():
            cross_copy(k).wait_send()
            outer_copy(k).wait_send()

        side_copy(k).wait_send()
        pair_copy(0, k).wait_send()
        pair_copy(1, k).wait_send()

    for k in range(chunks):
        held(k, sent)


def place_kernel(*refs):
    for source, target in zip(refs[:5], refs[5:]):
        target[...] = source[...]


def on_device_quad(
    n,
    known_inverse,
    first_factor,
    first_corner,
    first_ancestors,
    second_factor,
    second_link,
    second_corner,
    second_ancestors,
):
    groups, share, block = known_inverse.shape
    width = second_link.shape[0]
    hw, quarter = second_corner.shape[1], width // 4
    one, two = first_ancestors.shape[0], second_ancestors.shape[0]
    rows_all = one + two + 3 * (one // 4)
    chunks = rows_all // CHUNK
    f32, bf16 = jnp.float32, jnp.bfloat16
    anywhere = pl.BlockSpec(memory_space=pl.ANY)
    vmem = pl.BlockSpec(memory_space=pltpu.VMEM)
    square = jax.ShapeDtypeStruct((width, hw), f32)
    column = jax.ShapeDtypeStruct((block, hw), f32)
    results = pl.pallas_call(
        functools.partial(quad_kernel, n),
        out_shape=tuple(pltpu.VMEM(x.shape, x.dtype) for x in (column, square, column, square, square)),
        in_specs=[anywhere, anywhere, anywhere, vmem, anywhere, anywhere, anywhere, vmem],
        out_specs=(vmem,) * 5,
        scratch_shapes=[
            pltpu.VMEM((groups, share, block), f32),
            pltpu.VMEM((2, block, quarter), f32),
            pltpu.VMEM((3, 2 * RAILS, block, quarter), f32),
            pltpu.VMEM((block, one), f32),
            pltpu.VMEM((block, one), f32),
            pltpu.VMEM((block, one), f32),
            pltpu.VMEM((one + two, 2 * RAILS * block), bf16),
            pltpu.VMEM((rows_all, quarter), f32),
            pltpu.VMEM((rows_all, quarter), f32),
            pltpu.VMEM((rows_all, quarter), f32),
            pltpu.VMEM((rows_all, quarter), f32),
            pltpu.VMEM((4, rows_all, quarter), f32),
            pltpu.VMEM((width, width), f32),
            pltpu.VMEM((width, width), f32),
            pltpu.VMEM((width, hw), f32),
            pltpu.VMEM((2, width, width), bf16),
            pltpu.VMEM((one, width), f32),
            pltpu.VMEM((2, one, 2 * width), bf16),
            pltpu.VMEM((2, 2 * width, one), bf16),
            pltpu.VMEM((2, one, 2 * hw), bf16),
            pltpu.VMEM((2, one, one), bf16),
            pltpu.VMEM((2, 2, one // 2, one // 2), bf16),
            pltpu.SemaphoreType.DMA((8,)),
            pltpu.SemaphoreType.DMA((2,)),
            pltpu.SemaphoreType.DMA((3, 3)),
            pltpu.SemaphoreType.DMA((3, 3)),
            pltpu.SemaphoreType.DMA((2, chunks)),
            pltpu.SemaphoreType.DMA((chunks,)),
            pltpu.SemaphoreType.DMA((chunks,)),
            pltpu.SemaphoreType.DMA((chunks,)),
            pltpu.SemaphoreType.DMA((2, chunks)),
            pltpu.SemaphoreType.DMA((2, chunks)),
        ],
        compiler_params=pltpu.CompilerParams(collective_id=0, has_side_effects=True),
    )(
        known_inverse,
        first_factor,
        first_corner,
        first_ancestors.reshape(1, -1),
        second_factor,
        second_link,
        second_corner,
        second_ancestors.reshape(1, -1),
    )
    results = [pltpu.with_memory_space_constraint(x, pltpu.VMEM) for x in results]
    return pl.pallas_call(
        place_kernel,
        out_shape=(column, square, column, square, square),
        in_specs=[vmem] * 5,
        out_specs=(vmem,) * 5,
    )(*results)


def solution(mesh):
    def on_device(*args):
        n = mesh.shape["row"]
        groups, share, block = args[0].shape
        width = args[5].shape[0]
        one, two = args[3].shape[0], args[7].shape[0]
        held = 4 * (one + two + 3 * (one // 4)) * (width // 4) * 9 + 16 * one * (width + one)
        fits = (
            mesh.shape["col"] == 2
            and n == LEVELS * RAILS
            and groups == n
            and block == 2 * share
            and block % 128 == 0
            and one == width
            and width % 512 == 0
            and two % 128 == 0
            and held <= VMEM_FOR_WHOLE
        )
        return on_device_quad(n, *args) if fits else on_device_collectives(*args)

    return jax.shard_map(
        on_device,
        mesh=mesh,
        in_specs=(
            P("pole", "col", "row"),
            P(("pole", "row"), None),
            P("pole", None),
            P("pole"),
            P(("pole", "row"), None),
            P("pole", None),
            P("pole", "col"),
            P("pole"),
        ),
        out_specs=(
            P(("pole", "row"), "col"),
            P("pole", "col"),
            P(("pole", "row"), "col"),
            P("pole", "col"),
            P("pole", "col"),
        ),
        check_vma=False,
    )
```

```python
import functools

import jax
import jax.numpy as jnp
from jax import lax
from jax.experimental import pallas as pl
from jax.experimental.pallas import tpu as pltpu
from jax.sharding import PartitionSpec as P

HIGH = lax.Precision.HIGHEST
MESH = pl.DeviceIdType.MESH
RAILS = 2
LEVELS = 4
CHUNK = 128
LAG = 3
RAW_TWO = (0, 0)
RAW_K = (2, 2)
VMEM_FOR_WHOLE = 20 * 2**20
GRANT = 57 * 2**20


def product(left, right):
    return jnp.dot(left, right, precision=HIGH, preferred_element_type=jnp.float32)


def transposed_product(left, right):
    return lax.dot_general(
        left, right, (((0,), (0,)), ((), ())), precision=HIGH, preferred_element_type=jnp.float32
    )


def local_mask(ancestors, row_start, block_rows):
    global_rows = row_start + jnp.arange(block_rows, dtype=jnp.int32)
    return jnp.any(ancestors[:, None] == global_rows[None, :], axis=0).astype(jnp.float32)[:, None]


def on_device_collectives(
    known_inverse,
    first_factor,
    first_corner,
    first_ancestors,
    second_factor,
    second_link,
    second_corner,
    second_ancestors,
):
    groups, share_rows, block_rows = known_inverse.shape
    half_width = second_corner.shape[1]
    col_index = lax.axis_index("col")
    row_start = lax.axis_index("row") * block_rows
    first_mask = local_mask(first_ancestors, row_start, block_rows)
    second_mask = local_mask(second_ancestors, row_start, block_rows)
    first_masked = first_factor * first_mask
    second_masked = second_factor * second_mask
    share_start = col_index * share_rows
    first_piece = lax.dynamic_slice_in_dim(first_masked, share_start, share_rows, 0)
    second_piece = lax.dynamic_slice_in_dim(second_masked, share_start, share_rows, 0)
    columns = known_inverse.reshape(groups * share_rows, block_rows)

    def add_piece(piece):
        return transposed_product(columns, piece)

    first_partial = add_piece(lax.all_gather(first_piece, "row", axis=0, tiled=True))
    second_partial = add_piece(lax.all_gather(second_piece, "row", axis=0, tiled=True))
    first_image = lax.psum_scatter(first_partial, "col", scatter_dimension=1, tiled=True)
    first_column = -(first_image * first_mask)
    first_full = lax.all_gather(first_column, "col", axis=1, tiled=True)
    diagonal_partial = transposed_product(first_masked, first_column)
    corner_half = lax.dynamic_slice_in_dim(first_corner, col_index * half_width, half_width, 1)
    first_diagonal = corner_half - lax.psum(diagonal_partial, "row")
    diagonal_full = lax.all_gather(first_diagonal, "col", axis=1, tiled=True)
    second_image = lax.psum_scatter(second_partial, "col", scatter_dimension=1, tiled=True)
    link_half = lax.dynamic_slice_in_dim(second_link, col_index * half_width, half_width, 1)
    second_column = -((second_image + product(first_full, link_half)) * second_mask)
    second_half = lax.dynamic_slice_in_dim(second_masked, col_index * half_width, half_width, 1)
    cross_partial = transposed_product(first_full, second_half)
    closing_partial = transposed_product(second_masked, second_column)
    cross_total, closing_total = lax.psum((cross_partial, closing_partial), "row")
    second_cross = -(cross_total + product(diagonal_full, link_half))
    second_diagonal = second_corner - closing_total - transposed_product(second_link, second_cross)
    return (first_column, first_diagonal, second_column, second_cross, second_diagonal)


def split(value):
    high = value.astype(jnp.bfloat16)
    return high, (value - high.astype(jnp.float32)).astype(jnp.bfloat16)


def dot(left, right):
    return jnp.dot(left, right, preferred_element_type=jnp.float32)


def dot3(left, right):
    (left_high, left_low), (right_high, right_low) = left, right
    return dot(left_high, right_high) + (dot(left_low, right_high) + dot(left_high, right_low))


def quad_kernel(
    n,
    known,
    factor_one,
    corner_one,
    ancestors_one,
    factor_two,
    link,
    corner_two,
    ancestors_two,
    diagonal_one,
    cross_two,
    diagonal_two,
    k_full,
    mine_split,
    both_t,
    grown,
    masks,
    k_raw,
    stage,
    raw,
    k_part,
    k_peer,
    select,
    spread,
    pair,
    quad,
    inward,
    outward,
    total,
    link_buf,
    corner_buf,
    corner_two_buf,
    link_split,
    reduced,
    both,
    k_split,
    local_sem,
    k_sem,
    raw_send,
    raw_recv,
    hop_send,
    hop_recv,
    side_send,
    side_recv,
    pair_send,
    pair_recv,
):
    f32, bf16 = jnp.float32, jnp.bfloat16
    groups, share, block = k_raw.shape
    width = link_buf.shape[0]
    hw, quarter = width // 2, width // 4
    one, two = ancestors_one.shape[1], ancestors_two.shape[1]
    rows_all = pair.shape[0]
    chunks = rows_all // CHUNK
    part = one // 4
    k_start = one + two
    common = (k_start + 2 * part) // CHUNK
    pair_rows = RAILS * block

    me_row, me_col = lax.axis_index("row"), lax.axis_index("col")
    level, rail = me_row // RAILS, lax.rem(me_row, RAILS)
    parity = lax.rem(level, 2)
    mate_level = level + 1 - 2 * parity
    other_rail, other_col = 1 - rail, 1 - me_col
    my_quarter = 2 * me_col + rail
    side_quarter = 2 * me_col + other_rail
    my_place = RAILS * parity + rail
    inner = jnp.logical_and(level > 0, level < LEVELS - 1)
    outer = jnp.logical_not(inner)
    extra = me_col == 1
    side_row = level * RAILS + other_rail
    mate_row = mate_level * RAILS + rail
    slant_row = mate_level * RAILS + other_rail
    across_row = (LEVELS - 1 - level) * RAILS + rail

    barrier = pltpu.get_barrier_semaphore()

    def greet(**place):
        pl.semaphore_signal(barrier, inc=1, device_id=place, device_id_type=MESH)

    greet(row=slant_row)
    greet(row=mate_row)
    greet(row=side_row)
    greet(col=other_col)

    @pl.when(inner)
    def _():
        greet(row=across_row)

    count = [0]

    def local(src, dst):
        copy = pltpu.make_async_copy(src, dst, local_sem.at[count[0]])
        count[0] += 1
        copy.start()
        return copy

    def lanes(which):
        return pl.ds(pl.multiple_of(which * quarter, 128), quarter)

    f_copies = [
        [
            local(factor.at[:, lanes(side_quarter)], stage.at[i]),
            local(factor.at[:, lanes(my_quarter)], raw.at[i, my_place]),
        ]
        for i, factor in enumerate((factor_one, factor_two))
    ]
    k_own = local(known, k_raw)
    rest = [local(link, link_buf), local(corner_one, corner_buf), local(corner_two, corner_two_buf)]

    def remote(src, dst, send, recv, **place):
        return pltpu.make_async_remote_copy(
            src_ref=src, dst_ref=dst, send_sem=send, recv_sem=recv, device_id=place, device_id_type=MESH
        )

    def raw_copy(kind, i):
        if kind == 0:
            src = raw.at[i, my_place]
        else:
            src = stage.at[i] if i < 2 else k_full.at[:, lanes(side_quarter)]
        row = (mate_row, side_row, slant_row)[kind]
        return remote(src, raw.at[i, my_place], raw_send.at[kind, i], raw_recv.at[kind, i], row=row)

    def send_raw(i):
        @pl.when(outer)
        def _():
            raw_copy(0, i).start()
            raw_copy(2, i).start()

        raw_copy(1, i).start()

    def k_copy():
        return remote(k_part, k_peer, k_sem.at[0], k_sem.at[1], col=other_col)

    def rows_of(k):
        return pl.ds(pl.multiple_of(k * CHUNK, CHUNK), CHUNK)

    def cross_copy(k):
        at = rows_of(k)
        return remote(quad.at[at], inward.at[at], hop_send.at[0, k], hop_recv.at[k], row=across_row)

    def outer_copy(k):
        at = rows_of(k)
        return remote(outward.at[at], inward.at[at], hop_send.at[1, k], hop_recv.at[k], row=mate_row)

    def side_copy(k):
        at = total.at[my_quarter, rows_of(k)]
        return remote(at, at, side_send.at[k], side_recv.at[k], row=side_row)

    def pair_copy(which, k):
        at = total.at[my_quarter if which == 0 else side_quarter, rows_of(k)]
        return remote(at, at, pair_send.at[which, k], pair_recv.at[which, k], col=other_col)

    def held(k, act):
        if k >= common:

            @pl.when(extra)
            def _():
                act(k)
        else:
            act(k)

    def numbers(ancestors):
        wide = jnp.broadcast_to(ancestors[...].astype(f32), (128, ancestors.shape[1]))
        return wide.T

    def selection(column):
        shape = (column.shape[0], 2 * pair_rows)
        lane = lax.broadcasted_iota(jnp.int32, shape, 1) + (level // 2) * (2 * pair_rows)
        repeated = jnp.concatenate([column] * (2 * pair_rows // 128), axis=1)
        return jnp.where(repeated == lane.astype(f32), 1.0, 0.0).astype(bf16)

    column = numbers(ancestors_one)
    select[:one, :] = selection(column)
    select[one:, :] = selection(numbers(ancestors_two))
    k_split[...] = jnp.zeros_like(k_split)
    same = jnp.concatenate([column] * (two // 128), axis=1) == ancestors_two[...].astype(f32)
    spread[...] = jnp.where(same, 1.0, 0.0).astype(bf16)

    for copies in f_copies:
        for copy in copies:
            copy.wait()
    pl.semaphore_wait(barrier, 4 + inner.astype(jnp.int32))
    send_raw(0)

    k_own.wait()
    at = (
        lax.broadcasted_iota(jnp.int32, (groups, share, one), 0) * block
        + lax.broadcasted_iota(jnp.int32, (groups, share, one), 1)
        + me_col * share
    )
    pick = jnp.where(at == ancestors_one[...].reshape(1, 1, one), 1.0, 0.0).astype(bf16)
    k_high, k_low = split(k_raw[...].reshape(groups * share, block).T)
    stacked = dot(jnp.concatenate([k_high, k_low], axis=0), pick.reshape(groups * share, one))
    k_part[...] = stacked[:block] + stacked[block:]
    k_copy().start()

    def mine(ref, start):
        return ref[:, pl.ds(pl.multiple_of(start + me_col * hw, 128), hw)]

    for copy in rest:
        copy.wait()
    link_split[0], link_split[1] = split(link_buf[...])
    half_split = split(mine(link_buf, 0))
    corner_link = dot3(split(corner_buf[...]), half_split)
    cross_two[...] = -corner_link
    diagonal_one[...] = mine(corner_buf, 0)
    diagonal_two[...] = corner_two_buf[...] + dot3(split(link_buf[...].T), split(corner_link))

    def mask_of(ancestors):
        rows = me_row * block + lax.broadcasted_iota(jnp.int32, (block, ancestors.shape[1]), 0)
        found = jnp.max(jnp.where(rows == ancestors[...], 1.0, 0.0), axis=1, keepdims=True)
        return jnp.broadcast_to(found, (block, 128))

    masks[0], masks[1] = mask_of(ancestors_one), mask_of(ancestors_two)

    def halves(i, which):
        high, low = split(raw[i, pl.ds(which * RAILS, RAILS)].reshape(pair_rows, quarter))
        return jnp.concatenate([high, low], axis=1)

    def placed(which, value, start, size):
        columns = pl.ds(pl.multiple_of(which * pair_rows, 128), pair_rows)
        wide = dot(select[pl.ds(start, size), columns], value)
        return wide[:, :quarter] + wide[:, quarter:]

    pieces = (
        [(0, 0, one)],
        [(one, one, two)],
        [
            (k_start + i * part, pl.multiple_of(lax.rem(my_quarter + i, 4) * part, part), part)
            for i in range(3)
        ],
    )

    def add_pair(i):
        value = halves(i, parity)
        for to, start, size in pieces[i]:
            pair[to : to + size, :] = placed(parity, value, start, size)

    def add_quad(i):
        value = halves(i, 1 - parity)
        for to, start, size in pieces[i]:
            quad[to : to + size, :] = pair[to : to + size, :] + placed(1 - parity, value, start, size)
        for k in range(pieces[i][0][0] // CHUNK, (pieces[i][-1][0] + pieces[i][-1][2]) // CHUNK):
            held(k, lambda k: cross_copy(k).start())

    raw_copy(1, 0).wait_recv()
    add_pair(0)

    @pl.when(inner)
    def _():
        raw_copy(0, 0).wait_recv()
        raw_copy(2, 0).wait_recv()
        add_quad(0)

    send_raw(1)
    k_copy().wait_recv()
    k_full[...] = k_part[...] + k_peer[...]
    raw[2, my_place] = k_full[:, lanes(my_quarter)]
    send_raw(2)

    @pl.when(outer)
    def _():
        for i in (1, 2):
            raw_copy(1, i).wait_recv()
            add_pair(i)

    def inner_adds(i):
        @pl.when(inner)
        def _():
            for kind in range(3):
                raw_copy(kind, i).wait_recv()
            add_pair(i)
            add_quad(i)

    def far_event(k):
        cross_copy(k).wait_recv()
        at = rows_of(k)

        @pl.when(inner)
        def _():
            outward[at] = pair[at] + inward[at]
            total[my_quarter, at] = quad[at] + inward[at]
            outer_copy(k).start()

        @pl.when(outer)
        def _():
            total[my_quarter, at] = pair[at] + inward[at]

        side_copy(k).start()
        pair_copy(0, k).start()

    def relay(k):
        side_copy(k).wait_recv()
        pair_copy(1, k).start()

    def from_pair(first, last):
        for k in range(first // CHUNK, last // CHUNK):
            pair_copy(0, k).wait_recv()
            pair_copy(1, k).wait_recv()

    def keep(col, start, value, mine_too):
        cols, at = slice(col * hw, (col + 1) * hw), slice(start + col * hw, start + (col + 1) * hw)
        high, low = split(value)
        both_t[0, at, :], both_t[1, at, :] = split(value.T)
        if start == 0:
            both[0, :, cols], both[1, :, cols] = high, low
        if mine_too:
            to = slice(0, hw) if start == 0 else slice(hw, 2 * hw)
            mine_split[0, :, to], mine_split[1, :, to] = high, low

    def brought(col, rows):
        return jnp.concatenate([total[2 * col, rows, :], total[2 * col + 1, rows, :]], axis=1)

    def first_half(col, add, mine_too):
        keep(col, 0, brought(col, slice(0, one)), mine_too)
        cols = slice(col * hw, (col + 1) * hw)
        term = dot3((both[0, :, cols], both[1, :, cols]), (link_split[0, cols, :], link_split[1, cols, :]))
        reduced[...] = reduced[...] + term if add else term

    def second_half(col, mine_too):
        high, low = split(brought(col, slice(one, k_start)))
        value = dot(spread[...], high) + dot(spread[...], low) - reduced[:, col * hw : (col + 1) * hw]
        keep(col, width, value, mine_too)

    def put(row, col, value):
        at = (slice(row * part, (row + 1) * part), slice(col * part, (col + 1) * part))
        k_split[(0, *at)], k_split[(1, *at)] = split(value)

    def block_of(q, i):
        return total[q, k_start + i * part : k_start + (i + 1) * part, :]

    def put_diagonal(col):
        for q in (2 * col, 2 * col + 1):
            put(q, q, block_of(q, 0))

    def put_others():
        for q in (2, 3):
            for i in (1, 2):
                value = block_of(q, i)
                put((q + i) % 4, q, value)
                put(q, (q + i) % 4, value.T)

    def grow(half):
        rows = slice(half * (one // 2), (half + 1) * (one // 2))
        reduced[rows, :] = dot3((k_split[0, rows], k_split[1, rows]), (mine_split[0], mine_split[1]))

    def plan(col):
        mine_chunks = common if col == 0 else chunks
        ahead, before = one // CHUNK, k_start // CHUNK
        for k in range(mine_chunks):
            far_event(k)
            if k == RAW_TWO[col]:
                inner_adds(1)
            if k == RAW_K[col]:
                inner_adds(2)
            if col == 0 and k == ahead:
                from_pair(0, one)
                first_half(1, False, False)
            if col == 0 and k == min(ahead + LAG, mine_chunks - 1):
                first_half(0, True, True)
            if k >= LAG:
                relay(k - LAG)
            if col == 1 and k == ahead + LAG - 1:
                first_half(1, False, True)
        left = list(range(mine_chunks - LAG, mine_chunks))
        if col == 0:
            from_pair(one, k_start)
            second_half(1, False)
            for k in left:
                if k < before:
                    relay(k)
            second_half(0, True)
            later = [k for k in left if k >= before]
            for k in later[: (len(later) + 1) // 2]:
                relay(k)
            from_pair(k_start, rows_all)
            put_diagonal(1)
            put_others()
            put_diagonal(0)
            grow(0)
            for k in later[(len(later) + 1) // 2 :]:
                relay(k)
            grow(1)
        else:
            for k in left:
                if k < common:
                    relay(k)
            from_pair(0, one)
            first_half(0, True, False)
            second_half(1, True)
            for k in left:
                if k >= common:
                    relay(k)
            put_diagonal(1)
            put_others()
            from_pair(one, k_start)
            second_half(0, False)
            from_pair(k_start, k_start + part)
            put_diagonal(0)
            grow(0)
            grow(1)
            from_pair(k_start + part, k_start + 2 * part)

    for col in range(2):
        pl.when(me_col == col)(functools.partial(plan, col))

    def rows_at(q):
        return slice(q * part, (q + 1) * part)

    def mine_at(q):
        return mine_split[0, rows_at(q)], mine_split[1, rows_at(q)]

    lower = split(jnp.concatenate([block_of(0, 1).T, block_of(1, 1)], axis=0))
    middle = split(jnp.concatenate([block_of(0, 1), block_of(1, 1).T], axis=1))
    ends = tuple(jnp.concatenate(both_ends, axis=0) for both_ends in zip(mine_at(0), mine_at(2)))
    outer_term = dot3(lower, mine_at(1))
    middle_term = dot3(middle, ends)
    for q, term in ((3, None), (0, outer_term[:part]), (2, outer_term[part:]), (1, middle_term)):
        value = reduced[rows_at(q), :] if term is None else reduced[rows_at(q), :] + term
        grown[0, rows_at(q)], grown[1, rows_at(q)] = split(value)

    for i in range(3):
        raw_copy(1, i).wait_send()
    k_copy().wait_send()

    @pl.when(outer)
    def _():
        for i in range(3):
            raw_copy(0, i).wait_send()
            raw_copy(2, i).wait_send()

    def sent(k):
        @pl.when(inner)
        def _():
            cross_copy(k).wait_send()
            outer_copy(k).wait_send()

        side_copy(k).wait_send()
        pair_copy(0, k).wait_send()
        pair_copy(1, k).wait_send()

    for k in range(chunks):
        held(k, sent)


def closing_kernel(
    diagonal_one,
    cross_two,
    diagonal_two,
    k_full,
    mine_split,
    both_t,
    grown,
    masks,
    column_one_out,
    diagonal_one_out,
    column_two_out,
    cross_two_out,
    diagonal_two_out,
    squares,
    columns,
    sem,
):
    width = diagonal_one.shape[0]
    hw = diagonal_one.shape[1]
    copies = []

    def out(src, dst):
        copy = pltpu.make_async_copy(src, dst, sem.at[len(copies)])
        copy.start()
        copies.append(copy)

    sums = ((diagonal_one, 0, 0, diagonal_one_out), (cross_two, 0, hw, cross_two_out), (diagonal_two, width, hw, diagonal_two_out))
    for i, (base, row, col, target) in enumerate(sums):
        rows, cols = slice(row, row + width), slice(col, col + hw)
        squares[i] = base[...] + dot3((both_t[0, rows], both_t[1, rows]), (grown[0, :, cols], grown[1, :, cols]))
        out(squares.at[i], target)
    image = dot3(split(k_full[...]), (mine_split[0], mine_split[1]))
    for i, target in enumerate((column_one_out, column_two_out)):
        mask = jnp.concatenate([masks[i]] * (hw // 128), axis=1)
        columns[i] = -(image[:, i * hw : (i + 1) * hw] * mask)
        out(columns.at[i], target)
    for copy in copies:
        copy.wait()


def on_device_quad(
    n,
    known_inverse,
    first_factor,
    first_corner,
    first_ancestors,
    second_factor,
    second_link,
    second_corner,
    second_ancestors,
):
    groups, share, block = known_inverse.shape
    width = second_link.shape[0]
    hw, quarter = second_corner.shape[1], width // 4
    one, two = first_ancestors.shape[0], second_ancestors.shape[0]
    rows_all = one + two + 3 * (one // 4)
    chunks = rows_all // CHUNK
    f32, bf16 = jnp.float32, jnp.bfloat16
    anywhere = pl.BlockSpec(memory_space=pltpu.HBM)
    vmem = pl.BlockSpec(memory_space=pltpu.VMEM)
    square = jax.ShapeDtypeStruct((width, hw), f32)
    column = jax.ShapeDtypeStruct((block, hw), f32)
    passed = (
        square,
        square,
        square,
        jax.ShapeDtypeStruct((block, one), f32),
        jax.ShapeDtypeStruct((2, one, 2 * hw), bf16),
        jax.ShapeDtypeStruct((2, 2 * width, one), bf16),
        jax.ShapeDtypeStruct((2, one, 2 * hw), bf16),
        jax.ShapeDtypeStruct((2, block, 128), f32),
    )
    results = pl.pallas_call(
        functools.partial(quad_kernel, n),
        out_shape=tuple(pltpu.VMEM(x.shape, x.dtype) for x in passed),
        in_specs=[anywhere, anywhere, anywhere, vmem, anywhere, anywhere, anywhere, vmem],
        out_specs=(vmem,) * len(passed),
        scratch_shapes=[
            pltpu.VMEM((groups, share, block), f32),
            pltpu.VMEM((2, block, quarter), f32),
            pltpu.VMEM((3, 2 * RAILS, block, quarter), f32),
            pltpu.VMEM((block, one), f32),
            pltpu.VMEM((block, one), f32),
            pltpu.VMEM((one + two, 2 * RAILS * block), bf16),
            pltpu.VMEM((one, two), bf16),
            pltpu.VMEM((rows_all, quarter), f32),
            pltpu.VMEM((rows_all, quarter), f32),
            pltpu.VMEM((rows_all, quarter), f32),
            pltpu.VMEM((rows_all, quarter), f32),
            pltpu.VMEM((4, rows_all, quarter), f32),
            pltpu.VMEM((width, width), f32),
            pltpu.VMEM((width, width), f32),
            pltpu.VMEM((width, hw), f32),
            pltpu.VMEM((2, width, width), bf16),
            pltpu.VMEM((one, width), f32),
            pltpu.VMEM((2, one, width), bf16),
            pltpu.VMEM((2, one, one), bf16),
            pltpu.SemaphoreType.DMA((8,)),
            pltpu.SemaphoreType.DMA((2,)),
            pltpu.SemaphoreType.DMA((3, 3)),
            pltpu.SemaphoreType.DMA((3, 3)),
            pltpu.SemaphoreType.DMA((2, chunks)),
            pltpu.SemaphoreType.DMA((chunks,)),
            pltpu.SemaphoreType.DMA((chunks,)),
            pltpu.SemaphoreType.DMA((chunks,)),
            pltpu.SemaphoreType.DMA((2, chunks)),
            pltpu.SemaphoreType.DMA((2, chunks)),
        ],
        compiler_params=pltpu.CompilerParams(
            collective_id=0, has_side_effects=True, vmem_limit_bytes=GRANT
        ),
    )(
        known_inverse,
        first_factor,
        first_corner,
        first_ancestors.reshape(1, -1),
        second_factor,
        second_link,
        second_corner,
        second_ancestors.reshape(1, -1),
    )
    results = [pltpu.with_memory_space_constraint(x, pltpu.VMEM) for x in results]
    return pl.pallas_call(
        closing_kernel,
        out_shape=(column, square, column, square, square),
        in_specs=[vmem] * len(passed),
        out_specs=(anywhere,) * 5,
        scratch_shapes=[
            pltpu.VMEM((3, width, hw), f32),
            pltpu.VMEM((2, block, hw), f32),
            pltpu.SemaphoreType.DMA((5,)),
        ],
        compiler_params=pltpu.CompilerParams(vmem_limit_bytes=GRANT),
    )(*results)


def solution(mesh):
    def on_device(*args):
        n = mesh.shape["row"]
        groups, share, block = args[0].shape
        width = args[5].shape[0]
        one, two = args[3].shape[0], args[7].shape[0]
        held = 4 * (one + two + 3 * (one // 4)) * (width // 4) * 9 + 16 * one * (width + one)
        fits = (
            mesh.shape["col"] == 2
            and n == LEVELS * RAILS
            and groups == n
            and block == 2 * share
            and block % 128 == 0
            and one == width
            and width % 512 == 0
            and two % 128 == 0
            and held <= VMEM_FOR_WHOLE
        )
        return on_device_quad(n, *args) if fits else on_device_collectives(*args)

    return jax.shard_map(
        on_device,
        mesh=mesh,
        in_specs=(
            P("pole", "col", "row"),
            P(("pole", "row"), None),
            P("pole", None),
            P("pole"),
            P(("pole", "row"), None),
            P("pole", None),
            P("pole", "col"),
            P("pole"),
        ),
        out_specs=(
            P(("pole", "row"), "col"),
            P("pole", "col"),
            P(("pole", "row"), "col"),
            P("pole", "col"),
            P("pole", "col"),
        ),
        check_vma=False,
    )
```

```python
import functools

import jax
import jax.numpy as jnp
from jax import lax
from jax.experimental import pallas as pl
from jax.experimental.pallas import tpu as pltpu
from jax.sharding import PartitionSpec as P

HIGH = lax.Precision.HIGHEST
MESH = pl.DeviceIdType.MESH
RAILS = 2
LEVELS = 4
CHUNK = 128
LAG = 3
RAW_TWO = (0, 0)
RAW_K = (2, 2)
VMEM_FOR_WHOLE = 20 * 2**20
GRANT = 57 * 2**20


def product(left, right):
    return jnp.dot(left, right, precision=HIGH, preferred_element_type=jnp.float32)


def transposed_product(left, right):
    return lax.dot_general(
        left, right, (((0,), (0,)), ((), ())), precision=HIGH, preferred_element_type=jnp.float32
    )


def local_mask(ancestors, row_start, block_rows):
    global_rows = row_start + jnp.arange(block_rows, dtype=jnp.int32)
    return jnp.any(ancestors[:, None] == global_rows[None, :], axis=0).astype(jnp.float32)[:, None]


def on_device_collectives(
    known_inverse,
    first_factor,
    first_corner,
    first_ancestors,
    second_factor,
    second_link,
    second_corner,
    second_ancestors,
):
    groups, share_rows, block_rows = known_inverse.shape
    half_width = second_corner.shape[1]
    col_index = lax.axis_index("col")
    row_start = lax.axis_index("row") * block_rows
    first_mask = local_mask(first_ancestors, row_start, block_rows)
    second_mask = local_mask(second_ancestors, row_start, block_rows)
    first_masked = first_factor * first_mask
    second_masked = second_factor * second_mask
    share_start = col_index * share_rows
    first_piece = lax.dynamic_slice_in_dim(first_masked, share_start, share_rows, 0)
    second_piece = lax.dynamic_slice_in_dim(second_masked, share_start, share_rows, 0)
    columns = known_inverse.reshape(groups * share_rows, block_rows)

    def add_piece(piece):
        return transposed_product(columns, piece)

    first_partial = add_piece(lax.all_gather(first_piece, "row", axis=0, tiled=True))
    second_partial = add_piece(lax.all_gather(second_piece, "row", axis=0, tiled=True))
    first_image = lax.psum_scatter(first_partial, "col", scatter_dimension=1, tiled=True)
    first_column = -(first_image * first_mask)
    first_full = lax.all_gather(first_column, "col", axis=1, tiled=True)
    diagonal_partial = transposed_product(first_masked, first_column)
    corner_half = lax.dynamic_slice_in_dim(first_corner, col_index * half_width, half_width, 1)
    first_diagonal = corner_half - lax.psum(diagonal_partial, "row")
    diagonal_full = lax.all_gather(first_diagonal, "col", axis=1, tiled=True)
    second_image = lax.psum_scatter(second_partial, "col", scatter_dimension=1, tiled=True)
    link_half = lax.dynamic_slice_in_dim(second_link, col_index * half_width, half_width, 1)
    second_column = -((second_image + product(first_full, link_half)) * second_mask)
    second_half = lax.dynamic_slice_in_dim(second_masked, col_index * half_width, half_width, 1)
    cross_partial = transposed_product(first_full, second_half)
    closing_partial = transposed_product(second_masked, second_column)
    cross_total, closing_total = lax.psum((cross_partial, closing_partial), "row")
    second_cross = -(cross_total + product(diagonal_full, link_half))
    second_diagonal = second_corner - closing_total - transposed_product(second_link, second_cross)
    return (first_column, first_diagonal, second_column, second_cross, second_diagonal)


def split(value):
    high = value.astype(jnp.bfloat16)
    return high, (value - high.astype(jnp.float32)).astype(jnp.bfloat16)


def dot(left, right):
    return jnp.dot(left, right, preferred_element_type=jnp.float32)


def dot3(left, right):
    (left_high, left_low), (right_high, right_low) = left, right
    return dot(left_high, right_high) + (dot(left_low, right_high) + dot(left_high, right_low))


def quad_kernel(
    n,
    known,
    factor_one,
    corner_one,
    ancestors_one,
    factor_two,
    link,
    corner_two,
    ancestors_two,
    diagonal_one,
    cross_two,
    diagonal_two,
    k_full,
    mine_split,
    both_t,
    grown,
    masks,
    k_raw,
    stage,
    raw,
    k_part,
    k_peer,
    select,
    spread,
    pair,
    quad,
    inward,
    outward,
    total,
    link_buf,
    corner_buf,
    corner_two_buf,
    link_split,
    reduced,
    swelled,
    both,
    k_split,
    local_sem,
    k_sem,
    raw_send,
    raw_recv,
    hop_send,
    hop_recv,
    side_send,
    side_recv,
    pair_send,
    pair_recv,
):
    f32, bf16 = jnp.float32, jnp.bfloat16
    groups, share, block = k_raw.shape
    width = link_buf.shape[0]
    hw, quarter = width // 2, width // 4
    one, two = ancestors_one.shape[1], ancestors_two.shape[1]
    rows_all = pair.shape[0]
    chunks = rows_all // CHUNK
    part = one // 4
    k_start = one + two
    common = (k_start + 2 * part) // CHUNK
    pair_rows = RAILS * block

    me_row, me_col = lax.axis_index("row"), lax.axis_index("col")
    level, rail = me_row // RAILS, lax.rem(me_row, RAILS)
    parity = lax.rem(level, 2)
    mate_level = level + 1 - 2 * parity
    other_rail, other_col = 1 - rail, 1 - me_col
    my_quarter = 2 * me_col + rail
    side_quarter = 2 * me_col + other_rail
    my_place = RAILS * parity + rail
    inner = jnp.logical_and(level > 0, level < LEVELS - 1)
    outer = jnp.logical_not(inner)
    extra = me_col == 1
    side_row = level * RAILS + other_rail
    mate_row = mate_level * RAILS + rail
    slant_row = mate_level * RAILS + other_rail
    across_row = (LEVELS - 1 - level) * RAILS + rail

    barrier = pltpu.get_barrier_semaphore()

    def greet(**place):
        pl.semaphore_signal(barrier, inc=1, device_id=place, device_id_type=MESH)

    greet(row=slant_row)
    greet(row=mate_row)
    greet(row=side_row)
    greet(col=other_col)

    @pl.when(inner)
    def _():
        greet(row=across_row)

    count = [0]

    def local(src, dst):
        copy = pltpu.make_async_copy(src, dst, local_sem.at[count[0]])
        count[0] += 1
        copy.start()
        return copy

    def lanes(which):
        return pl.ds(pl.multiple_of(which * quarter, 128), quarter)

    f_copies = [
        [
            local(factor.at[:, lanes(side_quarter)], stage.at[i]),
            local(factor.at[:, lanes(my_quarter)], raw.at[i, my_place]),
        ]
        for i, factor in enumerate((factor_one, factor_two))
    ]
    k_own = local(known, k_raw)
    rest = [local(link, link_buf), local(corner_one, corner_buf), local(corner_two, corner_two_buf)]

    def remote(src, dst, send, recv, **place):
        return pltpu.make_async_remote_copy(
            src_ref=src, dst_ref=dst, send_sem=send, recv_sem=recv, device_id=place, device_id_type=MESH
        )

    def raw_copy(kind, i):
        if kind == 0:
            src = raw.at[i, my_place]
        else:
            src = stage.at[i] if i < 2 else k_full.at[:, lanes(side_quarter)]
        row = (mate_row, side_row, slant_row)[kind]
        return remote(src, raw.at[i, my_place], raw_send.at[kind, i], raw_recv.at[kind, i], row=row)

    def send_raw(i):
        @pl.when(outer)
        def _():
            raw_copy(0, i).start()
            raw_copy(2, i).start()

        raw_copy(1, i).start()

    def k_copy():
        return remote(k_part, k_peer, k_sem.at[0], k_sem.at[1], col=other_col)

    def rows_of(k):
        return pl.ds(pl.multiple_of(k * CHUNK, CHUNK), CHUNK)

    def cross_copy(k):
        at = rows_of(k)
        return remote(quad.at[at], inward.at[at], hop_send.at[0, k], hop_recv.at[k], row=across_row)

    def outer_copy(k):
        at = rows_of(k)
        return remote(outward.at[at], inward.at[at], hop_send.at[1, k], hop_recv.at[k], row=mate_row)

    def side_copy(k):
        at = total.at[my_quarter, rows_of(k)]
        return remote(at, at, side_send.at[k], side_recv.at[k], row=side_row)

    def pair_copy(which, k):
        at = total.at[my_quarter if which == 0 else side_quarter, rows_of(k)]
        return remote(at, at, pair_send.at[which, k], pair_recv.at[which, k], col=other_col)

    def held(k, act):
        if k >= common:

            @pl.when(extra)
            def _():
                act(k)
        else:
            act(k)

    def numbers(ancestors):
        wide = jnp.broadcast_to(ancestors[...].astype(f32), (128, ancestors.shape[1]))
        return wide.T

    def selection(column):
        shape = (column.shape[0], 2 * pair_rows)
        lane = lax.broadcasted_iota(jnp.int32, shape, 1) + (level // 2) * (2 * pair_rows)
        repeated = jnp.concatenate([column] * (2 * pair_rows // 128), axis=1)
        return jnp.where(repeated == lane.astype(f32), 1.0, 0.0).astype(bf16)

    column = numbers(ancestors_one)
    select[:one, :] = selection(column)
    select[one:, :] = selection(numbers(ancestors_two))
    k_split[...] = jnp.zeros_like(k_split)
    same = jnp.concatenate([column] * (two // 128), axis=1) == ancestors_two[...].astype(f32)
    spread[...] = jnp.where(same, 1.0, 0.0).astype(bf16)

    for copies in f_copies:
        for copy in copies:
            copy.wait()
    pl.semaphore_wait(barrier, 4 + inner.astype(jnp.int32))
    send_raw(0)

    k_own.wait()
    at = (
        lax.broadcasted_iota(jnp.int32, (groups, share, one), 0) * block
        + lax.broadcasted_iota(jnp.int32, (groups, share, one), 1)
        + me_col * share
    )
    pick = jnp.where(at == ancestors_one[...].reshape(1, 1, one), 1.0, 0.0).astype(bf16)
    k_high, k_low = split(k_raw[...].reshape(groups * share, block).T)
    stacked = dot(jnp.concatenate([k_high, k_low], axis=0), pick.reshape(groups * share, one))
    k_part[...] = stacked[:block] + stacked[block:]
    k_copy().start()

    def mine(ref, start):
        return ref[:, pl.ds(pl.multiple_of(start + me_col * hw, 128), hw)]

    for copy in rest:
        copy.wait()
    link_split[0], link_split[1] = split(link_buf[...])
    half_split = split(mine(link_buf, 0))
    corner_link = dot3(split(corner_buf[...]), half_split)
    cross_two[...] = -corner_link
    diagonal_one[...] = mine(corner_buf, 0)
    diagonal_two[...] = corner_two_buf[...] + dot3(split(link_buf[...].T), split(corner_link))

    def mask_of(ancestors):
        rows = me_row * block + lax.broadcasted_iota(jnp.int32, (block, ancestors.shape[1]), 0)
        found = jnp.max(jnp.where(rows == ancestors[...], 1.0, 0.0), axis=1, keepdims=True)
        return jnp.broadcast_to(found, (block, 128))

    masks[0], masks[1] = mask_of(ancestors_one), mask_of(ancestors_two)

    def halves(i, which):
        high, low = split(raw[i, pl.ds(which * RAILS, RAILS)].reshape(pair_rows, quarter))
        return jnp.concatenate([high, low], axis=1)

    def placed(which, value, start, size):
        columns = pl.ds(pl.multiple_of(which * pair_rows, 128), pair_rows)
        wide = dot(select[pl.ds(start, size), columns], value)
        return wide[:, :quarter] + wide[:, quarter:]

    pieces = (
        [(0, 0, one)],
        [(one, one, two)],
        [
            (k_start + i * part, pl.multiple_of(lax.rem(my_quarter + i, 4) * part, part), part)
            for i in range(3)
        ],
    )

    def add_pair(i):
        value = halves(i, parity)
        for to, start, size in pieces[i]:
            pair[to : to + size, :] = placed(parity, value, start, size)

    def add_quad(i):
        value = halves(i, 1 - parity)
        for to, start, size in pieces[i]:
            quad[to : to + size, :] = pair[to : to + size, :] + placed(1 - parity, value, start, size)
        for k in range(pieces[i][0][0] // CHUNK, (pieces[i][-1][0] + pieces[i][-1][2]) // CHUNK):
            held(k, lambda k: cross_copy(k).start())

    raw_copy(1, 0).wait_recv()
    add_pair(0)

    @pl.when(inner)
    def _():
        raw_copy(0, 0).wait_recv()
        raw_copy(2, 0).wait_recv()
        add_quad(0)

    send_raw(1)
    k_copy().wait_recv()
    k_full[...] = k_part[...] + k_peer[...]
    raw[2, my_place] = k_full[:, lanes(my_quarter)]
    send_raw(2)

    @pl.when(outer)
    def _():
        for i in (1, 2):
            raw_copy(1, i).wait_recv()
            add_pair(i)

    def inner_adds(i):
        @pl.when(inner)
        def _():
            for kind in range(3):
                raw_copy(kind, i).wait_recv()
            add_pair(i)
            add_quad(i)

    def far_event(k):
        cross_copy(k).wait_recv()
        at = rows_of(k)

        @pl.when(inner)
        def _():
            outward[at] = pair[at] + inward[at]
            total[my_quarter, at] = quad[at] + inward[at]
            outer_copy(k).start()

        @pl.when(outer)
        def _():
            total[my_quarter, at] = pair[at] + inward[at]

        side_copy(k).start()
        pair_copy(0, k).start()

    def relay(k):
        side_copy(k).wait_recv()
        pair_copy(1, k).start()

    def from_pair(first, last):
        for k in range(first // CHUNK, last // CHUNK):
            pair_copy(0, k).wait_recv()
            pair_copy(1, k).wait_recv()

    def keep(col, start, value, mine_too):
        cols, at = slice(col * hw, (col + 1) * hw), slice(start + col * hw, start + (col + 1) * hw)
        high, low = split(value)
        both_t[0, at, :], both_t[1, at, :] = split(value.T)
        if start == 0:
            both[0, :, cols], both[1, :, cols] = high, low
        if mine_too:
            to = slice(0, hw) if start == 0 else slice(hw, 2 * hw)
            mine_split[0, :, to], mine_split[1, :, to] = high, low

    def brought(col, rows):
        return jnp.concatenate([total[2 * col, rows, :], total[2 * col + 1, rows, :]], axis=1)

    def first_half(col, add, mine_too):
        keep(col, 0, brought(col, slice(0, one)), mine_too)
        cols = slice(col * hw, (col + 1) * hw)
        term = dot3((both[0, :, cols], both[1, :, cols]), (link_split[0, cols, :], link_split[1, cols, :]))
        reduced[...] = reduced[...] + term if add else term

    def second_half(col, mine_too):
        high, low = split(brought(col, slice(one, k_start)))
        value = dot(spread[...], high) + dot(spread[...], low) - reduced[:, col * hw : (col + 1) * hw]
        keep(col, width, value, mine_too)

    def put(row, col, value):
        at = (slice(row * part, (row + 1) * part), slice(col * part, (col + 1) * part))
        k_split[(0, *at)], k_split[(1, *at)] = split(value)

    def block_of(q, i):
        return total[q, k_start + i * part : k_start + (i + 1) * part, :]

    def put_blocks():
        for q in (2, 3):
            put(q, q, block_of(q, 0))
            for i in (1, 2):
                value = block_of(q, i)
                put((q + i) % 4, q, value)
                put(q, (q + i) % 4, value.T)

    def grow(half):
        rows = slice(half * (one // 2), (half + 1) * (one // 2))
        swelled[rows, :] = dot3((k_split[0, rows], k_split[1, rows]), (mine_split[0], mine_split[1]))

    def plan(col):
        mine_chunks = common if col == 0 else chunks
        ahead, before = one // CHUNK, k_start // CHUNK
        for k in range(mine_chunks):
            far_event(k)
            if k == RAW_TWO[col]:
                inner_adds(1)
            if k == RAW_K[col]:
                inner_adds(2)
            if col == 0 and k == ahead:
                from_pair(0, one)
                first_half(1, False, False)
            if col == 0 and k == min(ahead + LAG, mine_chunks - 1):
                first_half(0, True, True)
            if k >= LAG:
                relay(k - LAG)
            if col == 1 and k == ahead + LAG - 1:
                first_half(1, False, True)
        left = list(range(mine_chunks - LAG, mine_chunks))
        if col == 0:
            from_pair(one, k_start)
            second_half(1, False)
            for k in left:
                if k < before:
                    relay(k)
            second_half(0, True)
            later = [k for k in left if k >= before]
            for k in later[: (len(later) + 1) // 2]:
                relay(k)
            from_pair(k_start, rows_all)
            put_blocks()
            grow(0)
            for k in later[(len(later) + 1) // 2 :]:
                relay(k)
            grow(1)
        else:
            for k in left:
                if k < common:
                    relay(k)
            from_pair(0, one)
            first_half(0, True, False)
            second_half(1, True)
            for k in left:
                if k >= common:
                    relay(k)
            put_blocks()
            grow(0)
            grow(1)
            from_pair(one, k_start)
            second_half(0, False)
            from_pair(k_start, k_start + 2 * part)

    for col in range(2):
        pl.when(me_col == col)(functools.partial(plan, col))

    def rows_at(q):
        return slice(q * part, (q + 1) * part)

    def mine_at(q):
        return mine_split[0, rows_at(q)], mine_split[1, rows_at(q)]

    top = jnp.concatenate([block_of(0, 0), block_of(0, 1).T], axis=1)
    bottom = jnp.concatenate([block_of(0, 1), block_of(1, 0)], axis=1)
    two_rows = slice(0, 2 * part)
    corner = dot3(
        split(jnp.concatenate([top, bottom], axis=0)), (mine_split[0, two_rows], mine_split[1, two_rows])
    )
    below = dot3(split(block_of(1, 1)), mine_at(1))
    beside = dot3(split(block_of(1, 1).T), mine_at(2))
    for q, term in ((3, None), (0, corner[:part]), (1, corner[part:] + beside), (2, below)):
        value = swelled[rows_at(q), :] if term is None else swelled[rows_at(q), :] + term
        grown[0, rows_at(q)], grown[1, rows_at(q)] = split(value)

    for i in range(3):
        raw_copy(1, i).wait_send()
    k_copy().wait_send()

    @pl.when(outer)
    def _():
        for i in range(3):
            raw_copy(0, i).wait_send()
            raw_copy(2, i).wait_send()

    def sent(k):
        @pl.when(inner)
        def _():
            cross_copy(k).wait_send()
            outer_copy(k).wait_send()

        side_copy(k).wait_send()
        pair_copy(0, k).wait_send()
        pair_copy(1, k).wait_send()

    for k in range(chunks):
        held(k, sent)


def closing_kernel(
    diagonal_one,
    cross_two,
    diagonal_two,
    k_full,
    mine_split,
    both_t,
    grown,
    masks,
    column_one_out,
    diagonal_one_out,
    column_two_out,
    cross_two_out,
    diagonal_two_out,
    squares,
    columns,
    sem,
):
    width = diagonal_one.shape[0]
    hw = diagonal_one.shape[1]
    copies = []

    def out(src, dst):
        copy = pltpu.make_async_copy(src, dst, sem.at[len(copies)])
        copy.start()
        copies.append(copy)

    sums = ((diagonal_one, 0, 0, diagonal_one_out), (cross_two, 0, hw, cross_two_out), (diagonal_two, width, hw, diagonal_two_out))
    for i, (base, row, col, target) in enumerate(sums):
        rows, cols = slice(row, row + width), slice(col, col + hw)
        squares[i] = base[...] + dot3((both_t[0, rows], both_t[1, rows]), (grown[0, :, cols], grown[1, :, cols]))
        out(squares.at[i], target)
    image = dot3(split(k_full[...]), (mine_split[0], mine_split[1]))
    for i, target in enumerate((column_one_out, column_two_out)):
        mask = jnp.concatenate([masks[i]] * (hw // 128), axis=1)
        columns[i] = -(image[:, i * hw : (i + 1) * hw] * mask)
        out(columns.at[i], target)
    for copy in copies:
        copy.wait()


def on_device_quad(
    n,
    known_inverse,
    first_factor,
    first_corner,
    first_ancestors,
    second_factor,
    second_link,
    second_corner,
    second_ancestors,
):
    groups, share, block = known_inverse.shape
    width = second_link.shape[0]
    hw, quarter = second_corner.shape[1], width // 4
    one, two = first_ancestors.shape[0], second_ancestors.shape[0]
    rows_all = one + two + 3 * (one // 4)
    chunks = rows_all // CHUNK
    f32, bf16 = jnp.float32, jnp.bfloat16
    anywhere = pl.BlockSpec(memory_space=pltpu.HBM)
    vmem = pl.BlockSpec(memory_space=pltpu.VMEM)
    square = jax.ShapeDtypeStruct((width, hw), f32)
    column = jax.ShapeDtypeStruct((block, hw), f32)
    passed = (
        square,
        square,
        square,
        jax.ShapeDtypeStruct((block, one), f32),
        jax.ShapeDtypeStruct((2, one, 2 * hw), bf16),
        jax.ShapeDtypeStruct((2, 2 * width, one), bf16),
        jax.ShapeDtypeStruct((2, one, 2 * hw), bf16),
        jax.ShapeDtypeStruct((2, block, 128), f32),
    )
    results = pl.pallas_call(
        functools.partial(quad_kernel, n),
        out_shape=tuple(pltpu.VMEM(x.shape, x.dtype) for x in passed),
        in_specs=[anywhere, anywhere, anywhere, vmem, anywhere, anywhere, anywhere, vmem],
        out_specs=(vmem,) * len(passed),
        scratch_shapes=[
            pltpu.VMEM((groups, share, block), f32),
            pltpu.VMEM((2, block, quarter), f32),
            pltpu.VMEM((3, 2 * RAILS, block, quarter), f32),
            pltpu.VMEM((block, one), f32),
            pltpu.VMEM((block, one), f32),
            pltpu.VMEM((one + two, 2 * RAILS * block), bf16),
            pltpu.VMEM((one, two), bf16),
            pltpu.VMEM((rows_all, quarter), f32),
            pltpu.VMEM((rows_all, quarter), f32),
            pltpu.VMEM((rows_all, quarter), f32),
            pltpu.VMEM((rows_all, quarter), f32),
            pltpu.VMEM((4, rows_all, quarter), f32),
            pltpu.VMEM((width, width), f32),
            pltpu.VMEM((width, width), f32),
            pltpu.VMEM((width, hw), f32),
            pltpu.VMEM((2, width, width), bf16),
            pltpu.VMEM((one, width), f32),
            pltpu.VMEM((one, 2 * hw), f32),
            pltpu.VMEM((2, one, width), bf16),
            pltpu.VMEM((2, one, one), bf16),
            pltpu.SemaphoreType.DMA((8,)),
            pltpu.SemaphoreType.DMA((2,)),
            pltpu.SemaphoreType.DMA((3, 3)),
            pltpu.SemaphoreType.DMA((3, 3)),
            pltpu.SemaphoreType.DMA((2, chunks)),
            pltpu.SemaphoreType.DMA((chunks,)),
            pltpu.SemaphoreType.DMA((chunks,)),
            pltpu.SemaphoreType.DMA((chunks,)),
            pltpu.SemaphoreType.DMA((2, chunks)),
            pltpu.SemaphoreType.DMA((2, chunks)),
        ],
        compiler_params=pltpu.CompilerParams(
            collective_id=0, has_side_effects=True, vmem_limit_bytes=GRANT
        ),
    )(
        known_inverse,
        first_factor,
        first_corner,
        first_ancestors.reshape(1, -1),
        second_factor,
        second_link,
        second_corner,
        second_ancestors.reshape(1, -1),
    )
    results = [pltpu.with_memory_space_constraint(x, pltpu.VMEM) for x in results]
    return pl.pallas_call(
        closing_kernel,
        out_shape=(column, square, column, square, square),
        in_specs=[vmem] * len(passed),
        out_specs=(anywhere,) * 5,
        scratch_shapes=[
            pltpu.VMEM((3, width, hw), f32),
            pltpu.VMEM((2, block, hw), f32),
            pltpu.SemaphoreType.DMA((5,)),
        ],
        compiler_params=pltpu.CompilerParams(vmem_limit_bytes=GRANT),
    )(*results)


def solution(mesh):
    def on_device(*args):
        n = mesh.shape["row"]
        groups, share, block = args[0].shape
        width = args[5].shape[0]
        one, two = args[3].shape[0], args[7].shape[0]
        held = 4 * (one + two + 3 * (one // 4)) * (width // 4) * 9 + 16 * one * (width + one)
        fits = (
            mesh.shape["col"] == 2
            and n == LEVELS * RAILS
            and groups == n
            and block == 2 * share
            and block % 128 == 0
            and one == width
            and width % 512 == 0
            and two % 128 == 0
            and held <= VMEM_FOR_WHOLE
        )
        return on_device_quad(n, *args) if fits else on_device_collectives(*args)

    return jax.shard_map(
        on_device,
        mesh=mesh,
        in_specs=(
            P("pole", "col", "row"),
            P(("pole", "row"), None),
            P("pole", None),
            P("pole"),
            P(("pole", "row"), None),
            P("pole", None),
            P("pole", "col"),
            P("pole"),
        ),
        out_specs=(
            P(("pole", "row"), "col"),
            P("pole", "col"),
            P(("pole", "row"), "col"),
            P("pole", "col"),
            P("pole", "col"),
        ),
        check_vma=False,
    )
```

```python
import functools

import jax
import jax.numpy as jnp
from jax import lax
from jax.experimental import pallas as pl
from jax.experimental.pallas import tpu as pltpu
from jax.sharding import PartitionSpec as P

HIGH = lax.Precision.HIGHEST
MESH = pl.DeviceIdType.MESH
RAILS = 2
LEVELS = 4
CHUNK = 128
LAG = 3
RAW_TWO = (0, 0)
RAW_K = (2, 2)
VMEM_FOR_WHOLE = 20 * 2**20
GRANT = 57 * 2**20


def product(left, right):
    return jnp.dot(left, right, precision=HIGH, preferred_element_type=jnp.float32)


def transposed_product(left, right):
    return lax.dot_general(
        left, right, (((0,), (0,)), ((), ())), precision=HIGH, preferred_element_type=jnp.float32
    )


def local_mask(ancestors, row_start, block_rows):
    global_rows = row_start + jnp.arange(block_rows, dtype=jnp.int32)
    return jnp.any(ancestors[:, None] == global_rows[None, :], axis=0).astype(jnp.float32)[:, None]


def on_device_collectives(
    known_inverse,
    first_factor,
    first_corner,
    first_ancestors,
    second_factor,
    second_link,
    second_corner,
    second_ancestors,
):
    groups, share_rows, block_rows = known_inverse.shape
    half_width = second_corner.shape[1]
    col_index = lax.axis_index("col")
    row_start = lax.axis_index("row") * block_rows
    first_mask = local_mask(first_ancestors, row_start, block_rows)
    second_mask = local_mask(second_ancestors, row_start, block_rows)
    first_masked = first_factor * first_mask
    second_masked = second_factor * second_mask
    share_start = col_index * share_rows
    first_piece = lax.dynamic_slice_in_dim(first_masked, share_start, share_rows, 0)
    second_piece = lax.dynamic_slice_in_dim(second_masked, share_start, share_rows, 0)
    columns = known_inverse.reshape(groups * share_rows, block_rows)

    def add_piece(piece):
        return transposed_product(columns, piece)

    first_partial = add_piece(lax.all_gather(first_piece, "row", axis=0, tiled=True))
    second_partial = add_piece(lax.all_gather(second_piece, "row", axis=0, tiled=True))
    first_image = lax.psum_scatter(first_partial, "col", scatter_dimension=1, tiled=True)
    first_column = -(first_image * first_mask)
    first_full = lax.all_gather(first_column, "col", axis=1, tiled=True)
    diagonal_partial = transposed_product(first_masked, first_column)
    corner_half = lax.dynamic_slice_in_dim(first_corner, col_index * half_width, half_width, 1)
    first_diagonal = corner_half - lax.psum(diagonal_partial, "row")
    diagonal_full = lax.all_gather(first_diagonal, "col", axis=1, tiled=True)
    second_image = lax.psum_scatter(second_partial, "col", scatter_dimension=1, tiled=True)
    link_half = lax.dynamic_slice_in_dim(second_link, col_index * half_width, half_width, 1)
    second_column = -((second_image + product(first_full, link_half)) * second_mask)
    second_half = lax.dynamic_slice_in_dim(second_masked, col_index * half_width, half_width, 1)
    cross_partial = transposed_product(first_full, second_half)
    closing_partial = transposed_product(second_masked, second_column)
    cross_total, closing_total = lax.psum((cross_partial, closing_partial), "row")
    second_cross = -(cross_total + product(diagonal_full, link_half))
    second_diagonal = second_corner - closing_total - transposed_product(second_link, second_cross)
    return (first_column, first_diagonal, second_column, second_cross, second_diagonal)


def split(value):
    high = value.astype(jnp.bfloat16)
    return high, (value - high.astype(jnp.float32)).astype(jnp.bfloat16)


def dot(left, right):
    return jnp.dot(left, right, preferred_element_type=jnp.float32)


def dot3(left, right):
    (left_high, left_low), (right_high, right_low) = left, right
    return dot(left_high, right_high) + (dot(left_low, right_high) + dot(left_high, right_low))


def quad_kernel(
    n,
    known,
    factor_one,
    corner_one,
    ancestors_one,
    factor_two,
    link,
    corner_two,
    ancestors_two,
    diagonal_one,
    cross_two,
    diagonal_two,
    k_full,
    mine_split,
    both_t,
    grown,
    masks,
    k_raw,
    stage,
    raw,
    k_part,
    k_peer,
    select,
    spread,
    pair,
    quad,
    inward,
    outward,
    total,
    link_buf,
    corner_buf,
    corner_two_buf,
    link_split,
    reduced,
    swelled,
    both,
    k_split,
    local_sem,
    k_sem,
    raw_send,
    raw_recv,
    hop_send,
    hop_recv,
    side_send,
    side_recv,
    pair_send,
    pair_recv,
):
    f32, bf16 = jnp.float32, jnp.bfloat16
    groups, share, block = k_raw.shape
    width = link_buf.shape[0]
    hw, quarter = width // 2, width // 4
    one, two = ancestors_one.shape[1], ancestors_two.shape[1]
    rows_all = pair.shape[0]
    chunks = rows_all // CHUNK
    part = one // 4
    k_start = one + two
    common = (k_start + 2 * part) // CHUNK
    pair_rows = RAILS * block

    me_row, me_col = lax.axis_index("row"), lax.axis_index("col")
    level, rail = me_row // RAILS, lax.rem(me_row, RAILS)
    parity = lax.rem(level, 2)
    mate_level = level + 1 - 2 * parity
    other_rail, other_col = 1 - rail, 1 - me_col
    my_quarter = 2 * me_col + rail
    side_quarter = 2 * me_col + other_rail
    my_place = RAILS * parity + rail
    inner = jnp.logical_and(level > 0, level < LEVELS - 1)
    outer = jnp.logical_not(inner)
    extra = me_col == 1
    side_row = level * RAILS + other_rail
    mate_row = mate_level * RAILS + rail
    slant_row = mate_level * RAILS + other_rail
    across_row = (LEVELS - 1 - level) * RAILS + rail

    barrier = pltpu.get_barrier_semaphore()

    def greet(**place):
        pl.semaphore_signal(barrier, inc=1, device_id=place, device_id_type=MESH)

    greet(row=slant_row)
    greet(row=mate_row)
    greet(row=side_row)
    greet(col=other_col)

    @pl.when(inner)
    def _():
        greet(row=across_row)

    count = [0]

    def local(src, dst):
        copy = pltpu.make_async_copy(src, dst, local_sem.at[count[0]])
        count[0] += 1
        copy.start()
        return copy

    def lanes(which):
        return pl.ds(pl.multiple_of(which * quarter, 128), quarter)

    f_copies = [
        [
            local(factor.at[:, lanes(side_quarter)], stage.at[i]),
            local(factor.at[:, lanes(my_quarter)], raw.at[i, my_place]),
        ]
        for i, factor in enumerate((factor_one, factor_two))
    ]
    k_own = local(known, k_raw)
    rest = [local(link, link_buf), local(corner_one, corner_buf), local(corner_two, corner_two_buf)]

    def remote(src, dst, send, recv, **place):
        return pltpu.make_async_remote_copy(
            src_ref=src, dst_ref=dst, send_sem=send, recv_sem=recv, device_id=place, device_id_type=MESH
        )

    def raw_copy(kind, i):
        if kind == 0:
            src = raw.at[i, my_place]
        else:
            src = stage.at[i] if i < 2 else k_full.at[:, lanes(side_quarter)]
        row = (mate_row, side_row, slant_row)[kind]
        return remote(src, raw.at[i, my_place], raw_send.at[kind, i], raw_recv.at[kind, i], row=row)

    def send_raw(i):
        @pl.when(outer)
        def _():
            raw_copy(0, i).start()
            raw_copy(2, i).start()

        raw_copy(1, i).start()

    def k_copy():
        return remote(k_part, k_peer, k_sem.at[0], k_sem.at[1], col=other_col)

    def rows_of(k):
        return pl.ds(pl.multiple_of(k * CHUNK, CHUNK), CHUNK)

    def cross_copy(k):
        at = rows_of(k)
        return remote(quad.at[at], inward.at[at], hop_send.at[0, k], hop_recv.at[k], row=across_row)

    def outer_copy(k):
        at = rows_of(k)
        return remote(outward.at[at], inward.at[at], hop_send.at[1, k], hop_recv.at[k], row=mate_row)

    def side_copy(k):
        at = total.at[my_quarter, rows_of(k)]
        return remote(at, at, side_send.at[k], side_recv.at[k], row=side_row)

    def pair_copy(which, k):
        at = total.at[my_quarter if which == 0 else side_quarter, rows_of(k)]
        return remote(at, at, pair_send.at[which, k], pair_recv.at[which, k], col=other_col)

    def held(k, act):
        if k >= common:

            @pl.when(extra)
            def _():
                act(k)
        else:
            act(k)

    def numbers(ancestors):
        wide = jnp.broadcast_to(ancestors[...].astype(f32), (128, ancestors.shape[1]))
        return wide.T

    def selection(column):
        shape = (column.shape[0], 2 * pair_rows)
        lane = lax.broadcasted_iota(jnp.int32, shape, 1) + (level // 2) * (2 * pair_rows)
        repeated = jnp.concatenate([column] * (2 * pair_rows // 128), axis=1)
        return jnp.where(repeated == lane.astype(f32), 1.0, 0.0).astype(bf16)

    column = numbers(ancestors_one)
    select[:one, :] = selection(column)
    select[one:, :] = selection(numbers(ancestors_two))
    k_split[...] = jnp.zeros_like(k_split)
    same = jnp.concatenate([column] * (two // 128), axis=1) == ancestors_two[...].astype(f32)
    spread[...] = jnp.where(same, 1.0, 0.0).astype(bf16)

    for copies in f_copies:
        for copy in copies:
            copy.wait()
    pl.semaphore_wait(barrier, 4 + inner.astype(jnp.int32))
    send_raw(0)

    k_own.wait()
    at = (
        lax.broadcasted_iota(jnp.int32, (groups, share, one), 0) * block
        + lax.broadcasted_iota(jnp.int32, (groups, share, one), 1)
        + me_col * share
    )
    pick = jnp.where(at == ancestors_one[...].reshape(1, 1, one), 1.0, 0.0).astype(bf16)
    k_high, k_low = split(k_raw[...].reshape(groups * share, block).T)
    stacked = dot(jnp.concatenate([k_high, k_low], axis=0), pick.reshape(groups * share, one))
    k_part[...] = stacked[:block] + stacked[block:]
    k_copy().start()

    def mine(ref, start):
        return ref[:, pl.ds(pl.multiple_of(start + me_col * hw, 128), hw)]

    for copy in rest:
        copy.wait()
    link_split[0], link_split[1] = split(link_buf[...])
    half_split = split(mine(link_buf, 0))
    corner_link = dot3(split(corner_buf[...]), half_split)
    cross_two[...] = -corner_link
    diagonal_one[...] = mine(corner_buf, 0)
    diagonal_two[...] = corner_two_buf[...] + dot3(split(link_buf[...].T), split(corner_link))

    def mask_of(ancestors):
        rows = me_row * block + lax.broadcasted_iota(jnp.int32, (block, ancestors.shape[1]), 0)
        found = jnp.max(jnp.where(rows == ancestors[...], 1.0, 0.0), axis=1, keepdims=True)
        return jnp.broadcast_to(found, (block, 128))

    masks[0], masks[1] = mask_of(ancestors_one), mask_of(ancestors_two)

    def halves(i, which):
        high, low = split(raw[i, pl.ds(which * RAILS, RAILS)].reshape(pair_rows, quarter))
        return jnp.concatenate([high, low], axis=1)

    def placed(which, value, start, size):
        columns = pl.ds(pl.multiple_of(which * pair_rows, 128), pair_rows)
        wide = dot(select[pl.ds(start, size), columns], value)
        return wide[:, :quarter] + wide[:, quarter:]

    pieces = (
        [(0, 0, one)],
        [(one, one, two)],
        [
            (k_start + i * part, pl.multiple_of(lax.rem(my_quarter + i, 4) * part, part), part)
            for i in range(3)
        ],
    )

    def add_pair(i):
        value = halves(i, parity)
        for to, start, size in pieces[i]:
            pair[to : to + size, :] = placed(parity, value, start, size)

    def add_quad(i):
        value = halves(i, 1 - parity)
        for to, start, size in pieces[i]:
            quad[to : to + size, :] = pair[to : to + size, :] + placed(1 - parity, value, start, size)
        for k in range(pieces[i][0][0] // CHUNK, (pieces[i][-1][0] + pieces[i][-1][2]) // CHUNK):
            held(k, lambda k: cross_copy(k).start())

    raw_copy(1, 0).wait_recv()
    send_raw(1)
    add_pair(0)

    @pl.when(inner)
    def _():
        raw_copy(0, 0).wait_recv()
        raw_copy(2, 0).wait_recv()
        add_quad(0)

    k_copy().wait_recv()
    k_full[...] = k_part[...] + k_peer[...]
    raw[2, my_place] = k_full[:, lanes(my_quarter)]
    send_raw(2)

    @pl.when(outer)
    def _():
        for i in (1, 2):
            raw_copy(1, i).wait_recv()
            add_pair(i)

    def inner_adds(i):
        @pl.when(inner)
        def _():
            for kind in range(3):
                raw_copy(kind, i).wait_recv()
            add_pair(i)
            add_quad(i)

    def far_event(k):
        cross_copy(k).wait_recv()
        at = rows_of(k)

        @pl.when(inner)
        def _():
            outward[at] = pair[at] + inward[at]
            total[my_quarter, at] = quad[at] + inward[at]
            outer_copy(k).start()

        @pl.when(outer)
        def _():
            total[my_quarter, at] = pair[at] + inward[at]

        side_copy(k).start()
        pair_copy(0, k).start()

    def relay(k):
        side_copy(k).wait_recv()
        pair_copy(1, k).start()

    def from_pair(first, last):
        for k in range(first // CHUNK, last // CHUNK):
            pair_copy(0, k).wait_recv()
            pair_copy(1, k).wait_recv()

    def keep(col, start, value, mine_too):
        cols, at = slice(col * hw, (col + 1) * hw), slice(start + col * hw, start + (col + 1) * hw)
        high, low = split(value)
        both_t[0, at, :], both_t[1, at, :] = split(value.T)
        if start == 0:
            both[0, :, cols], both[1, :, cols] = high, low
        if mine_too:
            to = slice(0, hw) if start == 0 else slice(hw, 2 * hw)
            mine_split[0, :, to], mine_split[1, :, to] = high, low

    def brought(col, rows):
        return jnp.concatenate([total[2 * col, rows, :], total[2 * col + 1, rows, :]], axis=1)

    def first_half(col, add, mine_too):
        keep(col, 0, brought(col, slice(0, one)), mine_too)
        cols = slice(col * hw, (col + 1) * hw)
        term = dot3((both[0, :, cols], both[1, :, cols]), (link_split[0, cols, :], link_split[1, cols, :]))
        reduced[...] = reduced[...] + term if add else term

    def second_half(col, mine_too):
        high, low = split(brought(col, slice(one, k_start)))
        value = dot(spread[...], high) + dot(spread[...], low) - reduced[:, col * hw : (col + 1) * hw]
        keep(col, width, value, mine_too)

    def put(row, col, value):
        at = (slice(row * part, (row + 1) * part), slice(col * part, (col + 1) * part))
        k_split[(0, *at)], k_split[(1, *at)] = split(value)

    def block_of(q, i):
        return total[q, k_start + i * part : k_start + (i + 1) * part, :]

    def put_blocks():
        for q in (2, 3):
            put(q, q, block_of(q, 0))
            for i in (1, 2):
                value = block_of(q, i)
                put((q + i) % 4, q, value)
                put(q, (q + i) % 4, value.T)

    def grow(half):
        rows = slice(half * (one // 2), (half + 1) * (one // 2))
        swelled[rows, :] = dot3((k_split[0, rows], k_split[1, rows]), (mine_split[0], mine_split[1]))

    def plan(col):
        mine_chunks = common if col == 0 else chunks
        ahead, before = one // CHUNK, k_start // CHUNK
        for k in range(mine_chunks):
            far_event(k)
            if k == RAW_TWO[col]:
                inner_adds(1)
            if k == RAW_K[col]:
                inner_adds(2)
            if col == 0 and k == ahead:
                from_pair(0, one)
                first_half(1, False, False)
            if col == 0 and k == min(ahead + LAG, mine_chunks - 1):
                first_half(0, True, True)
            if k >= LAG:
                relay(k - LAG)
            if col == 1 and k == ahead + LAG - 1:
                first_half(1, False, True)
        left = list(range(mine_chunks - LAG, mine_chunks))
        if col == 0:
            from_pair(one, k_start)
            second_half(1, False)
            for k in left:
                if k < before:
                    relay(k)
            second_half(0, True)
            later = [k for k in left if k >= before]
            for k in later[: (len(later) + 1) // 2]:
                relay(k)
            from_pair(k_start, rows_all)
            put_blocks()
            grow(0)
            for k in later[(len(later) + 1) // 2 :]:
                relay(k)
            grow(1)
        else:
            for k in left:
                if k < common:
                    relay(k)
            from_pair(0, one)
            first_half(0, True, False)
            second_half(1, True)
            for k in left:
                if k >= common:
                    relay(k)
            put_blocks()
            grow(0)
            grow(1)
            from_pair(one, k_start)
            second_half(0, False)
            from_pair(k_start, k_start + 2 * part)

    for col in range(2):
        pl.when(me_col == col)(functools.partial(plan, col))

    def rows_at(q):
        return slice(q * part, (q + 1) * part)

    def mine_at(q):
        return mine_split[0, rows_at(q)], mine_split[1, rows_at(q)]

    top = jnp.concatenate([block_of(0, 0), block_of(0, 1).T], axis=1)
    bottom = jnp.concatenate([block_of(0, 1), block_of(1, 0)], axis=1)
    two_rows = slice(0, 2 * part)
    corner = dot3(
        split(jnp.concatenate([top, bottom], axis=0)), (mine_split[0, two_rows], mine_split[1, two_rows])
    )
    below = dot3(split(block_of(1, 1)), mine_at(1))
    beside = dot3(split(block_of(1, 1).T), mine_at(2))
    for q, term in ((3, None), (0, corner[:part]), (1, corner[part:] + beside), (2, below)):
        value = swelled[rows_at(q), :] if term is None else swelled[rows_at(q), :] + term
        grown[0, rows_at(q)], grown[1, rows_at(q)] = split(value)

    for i in range(3):
        raw_copy(1, i).wait_send()
    k_copy().wait_send()

    @pl.when(outer)
    def _():
        for i in range(3):
            raw_copy(0, i).wait_send()
            raw_copy(2, i).wait_send()

    def sent(k):
        @pl.when(inner)
        def _():
            cross_copy(k).wait_send()
            outer_copy(k).wait_send()

        side_copy(k).wait_send()
        pair_copy(0, k).wait_send()
        pair_copy(1, k).wait_send()

    for k in range(chunks):
        held(k, sent)


def closing_kernel(
    diagonal_one,
    cross_two,
    diagonal_two,
    k_full,
    mine_split,
    both_t,
    grown,
    masks,
    column_one_out,
    diagonal_one_out,
    column_two_out,
    cross_two_out,
    diagonal_two_out,
    squares,
    columns,
    sem,
):
    width = diagonal_one.shape[0]
    hw = diagonal_one.shape[1]
    copies = []

    def out(src, dst):
        copy = pltpu.make_async_copy(src, dst, sem.at[len(copies)])
        copy.start()
        copies.append(copy)

    sums = ((diagonal_one, 0, 0, diagonal_one_out), (cross_two, 0, hw, cross_two_out), (diagonal_two, width, hw, diagonal_two_out))
    for i, (base, row, col, target) in enumerate(sums):
        rows, cols = slice(row, row + width), slice(col, col + hw)
        squares[i] = base[...] + dot3((both_t[0, rows], both_t[1, rows]), (grown[0, :, cols], grown[1, :, cols]))
        out(squares.at[i], target)
    image = dot3(split(k_full[...]), (mine_split[0], mine_split[1]))
    for i, target in enumerate((column_one_out, column_two_out)):
        mask = jnp.concatenate([masks[i]] * (hw // 128), axis=1)
        columns[i] = -(image[:, i * hw : (i + 1) * hw] * mask)
        out(columns.at[i], target)
    for copy in copies:
        copy.wait()


def on_device_quad(
    n,
    known_inverse,
    first_factor,
    first_corner,
    first_ancestors,
    second_factor,
    second_link,
    second_corner,
    second_ancestors,
):
    groups, share, block = known_inverse.shape
    width = second_link.shape[0]
    hw, quarter = second_corner.shape[1], width // 4
    one, two = first_ancestors.shape[0], second_ancestors.shape[0]
    rows_all = one + two + 3 * (one // 4)
    chunks = rows_all // CHUNK
    f32, bf16 = jnp.float32, jnp.bfloat16
    anywhere = pl.BlockSpec(memory_space=pltpu.HBM)
    vmem = pl.BlockSpec(memory_space=pltpu.VMEM)
    square = jax.ShapeDtypeStruct((width, hw), f32)
    column = jax.ShapeDtypeStruct((block, hw), f32)
    passed = (
        square,
        square,
        square,
        jax.ShapeDtypeStruct((block, one), f32),
        jax.ShapeDtypeStruct((2, one, 2 * hw), bf16),
        jax.ShapeDtypeStruct((2, 2 * width, one), bf16),
        jax.ShapeDtypeStruct((2, one, 2 * hw), bf16),
        jax.ShapeDtypeStruct((2, block, 128), f32),
    )
    results = pl.pallas_call(
        functools.partial(quad_kernel, n),
        out_shape=tuple(pltpu.VMEM(x.shape, x.dtype) for x in passed),
        in_specs=[anywhere, anywhere, anywhere, vmem, anywhere, anywhere, anywhere, vmem],
        out_specs=(vmem,) * len(passed),
        scratch_shapes=[
            pltpu.VMEM((groups, share, block), f32),
            pltpu.VMEM((2, block, quarter), f32),
            pltpu.VMEM((3, 2 * RAILS, block, quarter), f32),
            pltpu.VMEM((block, one), f32),
            pltpu.VMEM((block, one), f32),
            pltpu.VMEM((one + two, 2 * RAILS * block), bf16),
            pltpu.VMEM((one, two), bf16),
            pltpu.VMEM((rows_all, quarter), f32),
            pltpu.VMEM((rows_all, quarter), f32),
            pltpu.VMEM((rows_all, quarter), f32),
            pltpu.VMEM((rows_all, quarter), f32),
            pltpu.VMEM((4, rows_all, quarter), f32),
            pltpu.VMEM((width, width), f32),
            pltpu.VMEM((width, width), f32),
            pltpu.VMEM((width, hw), f32),
            pltpu.VMEM((2, width, width), bf16),
            pltpu.VMEM((one, width), f32),
            pltpu.VMEM((one, 2 * hw), f32),
            pltpu.VMEM((2, one, width), bf16),
            pltpu.VMEM((2, one, one), bf16),
            pltpu.SemaphoreType.DMA((8,)),
            pltpu.SemaphoreType.DMA((2,)),
            pltpu.SemaphoreType.DMA((3, 3)),
            pltpu.SemaphoreType.DMA((3, 3)),
            pltpu.SemaphoreType.DMA((2, chunks)),
            pltpu.SemaphoreType.DMA((chunks,)),
            pltpu.SemaphoreType.DMA((chunks,)),
            pltpu.SemaphoreType.DMA((chunks,)),
            pltpu.SemaphoreType.DMA((2, chunks)),
            pltpu.SemaphoreType.DMA((2, chunks)),
        ],
        compiler_params=pltpu.CompilerParams(
            collective_id=0, has_side_effects=True, vmem_limit_bytes=GRANT
        ),
    )(
        known_inverse,
        first_factor,
        first_corner,
        first_ancestors.reshape(1, -1),
        second_factor,
        second_link,
        second_corner,
        second_ancestors.reshape(1, -1),
    )
    results = [pltpu.with_memory_space_constraint(x, pltpu.VMEM) for x in results]
    return pl.pallas_call(
        closing_kernel,
        out_shape=(column, square, column, square, square),
        in_specs=[vmem] * len(passed),
        out_specs=(anywhere,) * 5,
        scratch_shapes=[
            pltpu.VMEM((3, width, hw), f32),
            pltpu.VMEM((2, block, hw), f32),
            pltpu.SemaphoreType.DMA((5,)),
        ],
        compiler_params=pltpu.CompilerParams(vmem_limit_bytes=GRANT),
    )(*results)


def solution(mesh):
    def on_device(*args):
        n = mesh.shape["row"]
        groups, share, block = args[0].shape
        width = args[5].shape[0]
        one, two = args[3].shape[0], args[7].shape[0]
        held = 4 * (one + two + 3 * (one // 4)) * (width // 4) * 9 + 16 * one * (width + one)
        fits = (
            mesh.shape["col"] == 2
            and n == LEVELS * RAILS
            and groups == n
            and block == 2 * share
            and block % 128 == 0
            and one == width
            and width % 512 == 0
            and two % 128 == 0
            and held <= VMEM_FOR_WHOLE
        )
        return on_device_quad(n, *args) if fits else on_device_collectives(*args)

    return jax.shard_map(
        on_device,
        mesh=mesh,
        in_specs=(
            P("pole", "col", "row"),
            P(("pole", "row"), None),
            P("pole", None),
            P("pole"),
            P(("pole", "row"), None),
            P("pole", None),
            P("pole", "col"),
            P("pole"),
        ),
        out_specs=(
            P(("pole", "row"), "col"),
            P("pole", "col"),
            P(("pole", "row"), "col"),
            P("pole", "col"),
            P("pole", "col"),
        ),
        check_vma=False,
    )
```
